256 devices in a mesh: groups: 2 (over y), fsdp: 32 (over z, core), expert: 4 (over x).
Axes of the slice: x: 4, y: 2, z: 16, core: 2. Of those that a mesh axis runs over, the one named last changes fastest.
The devices are a block of a 4x16x16 slice.
Arguments:
- queries: bfloat16 [4096, 2048], P(('groups', 'fsdp'), 'expert'), parts along dimension 0, may hold values from -14 to 14
- keys: bfloat16 [64, 2048, 512], P(('groups', 'fsdp'), None, 'expert'), parts along dimension 0, may hold values from -14 to 14
- values: bfloat16 [64, 2048, 512], P(('groups', 'fsdp'), None, 'expert'), parts along dimension 0, may hold values from -4 to 4
- out_weight: bfloat16 [2048, 4096], P('expert', 'fsdp'), may hold values from -0.5 to 0.5
- residual: bfloat16 [4096, 4096], P(('groups', 'fsdp')), parts along dimension 0, may hold values from -3 to 3
- norm_gain: float32 [4096], replicated, may hold values from 0.5 to 1.5
- route_ids: int32 [4096, 2], P(('groups', 'fsdp')), parts along dimension 0, may hold values from 0 to 7, as said below
- route_slots: int32 [4096, 2], P(('groups', 'fsdp')), parts along dimension 0, may hold values from 0 to 23, as said below
- route_weights: int32 [4096, 2], P(('groups', 'fsdp')), parts along dimension 0, may hold values from 1 to 65535, as said below
- w_gate: bfloat16 [8, 4096, 7168], P('expert', None, 'fsdp'), may hold values from -0.09375 to 0.09375
- w_up: bfloat16 [8, 4096, 7168], P('expert', None, 'fsdp'), may hold values from -0.09375 to 0.09375
- w_down: bfloat16 [8, 7168, 4096], P('expert', 'fsdp'), may hold values from -0.0625 to 0.0625
Outputs:
- layer_out: bfloat16 [4096, 4096], P(('groups', 'fsdp'), 'expert'), parts along dimension 0
The draws below stay inside these ranges and needn't reach their ends.
There are 2 independent parts, one for each index of `groups`. The reference program is written for one: setup_inputs(seed, part) draws one part's arguments, and reference() takes and returns one part's arrays. A program takes and returns all parts, laid end to end along the dimension named above; an argument that names none is the same for every part. Nothing has to cross between parts.
Inputs may be any that keep to these rules, and one draw needn't show every extreme that they name: `route_ids`: each row names two different experts. Among the rows of one block, no expert is named more than 24 times and no group of experts 2 g and 2 g + 1 more than 36 times; one expert, the same for all blocks, is named exactly 24 times in every block and its group exactly 36 times; every expert is named in every block. `route_slots`: within one block, the routes to one expert hold the slots 0 to their count - 1, each once. `route_weights`: the two entries of a row sum to 65536.
All inputs are finite; a program needn't handle non-finite values.
Results may differ from the reference program's by a relative error of at most 0.02.
Values may be sent and summed in bfloat16 or wider, within the bound.
A program may use at most 128 MiB of HBM per device.

```python
import jax
import jax.numpy as jnp
from jax import lax

D = 4096
HEADS = 16
KV_HEADS = 4
HEAD_DIM = 128
EXPERTS = 8
FFW = 7168
Q_BLOCK = 64
CTX = 2048
CAP = 24
GCAP = 36
SEQS = 32
TOKENS = 2048
N_FSDP = 32


def draw_queries(key, part):
    base_key = jax.random.fold_in(key, 5)
    shape = (SEQS, Q_BLOCK, KV_HEADS, HEADS // KV_HEADS, HEAD_DIM)
    base = jnp.clip(1.5 * jax.random.normal(base_key, shape, jnp.float32), -6.0, 6.0)
    return base.reshape(TOKENS, HEADS * HEAD_DIM).astype(jnp.bfloat16)


def draw_keys(key, part):
    base_key = jax.random.fold_in(key, 6)
    shape = (SEQS, CTX, KV_HEADS, HEAD_DIM)
    base = jnp.clip(jax.random.normal(base_key, shape, jnp.float32), -4.0, 4.0)
    return base.reshape(SEQS, CTX, KV_HEADS * HEAD_DIM).astype(jnp.bfloat16)


def shuffle_one(key):
    return jax.random.permutation(key, Q_BLOCK)


def route_table(key):
    sub = jax.random.fold_in(key, 11)
    busy_key, sum_key, turn_key, split_key, order_key = jax.random.split(sub, 5)
    busy = jax.random.randint(busy_key, (), 0, EXPERTS)
    busy_pair = busy // 2
    lower = 7 * Q_BLOCK // 16
    drawn = jax.random.randint(sum_key, (SEQS, 2), lower, GCAP + 1)
    third = 2 * Q_BLOCK - GCAP - drawn[:, 0] - drawn[:, 1]
    others = jnp.concatenate([drawn, third[:, None]], axis=1)
    turn = jax.random.randint(turn_key, (SEQS, 1), 0, 3)
    others = jnp.take_along_axis(others, (jnp.arange(3)[None, :] + turn) % 3, axis=1)
    pairs = jnp.arange(EXPERTS // 2)
    other_index = jnp.clip(pairs - (pairs > busy_pair).astype(jnp.int32), 0, 2)
    pair_sums = jnp.where(pairs[None, :] == busy_pair, GCAP, jnp.take(others, other_index, axis=1))
    low_split = jnp.maximum(pair_sums - CAP, 1)
    high_split = jnp.minimum(pair_sums - 1, CAP)
    evens = jax.random.randint(split_key, (SEQS, EXPERTS // 2), low_split, high_split + 1)
    busy_even = jnp.where(busy % 2 == 0, CAP, GCAP - CAP)
    evens = jnp.where(pairs[None, :] == busy_pair, busy_even, evens)
    counts = jnp.stack([evens, pair_sums - evens], axis=2).reshape(SEQS, EXPERTS)
    ends = jnp.cumsum(counts, axis=1)
    starts = ends - counts
    position = jnp.arange(2 * Q_BLOCK)
    owner = jnp.sum((ends[:, None, :] <= position[None, :, None]).astype(jnp.int32), axis=2)
    rank = position[None, :] - jnp.take_along_axis(starts, owner, axis=1)
    order = jax.vmap(shuffle_one)(jax.random.split(order_key, SEQS))
    pick = jnp.stack([order, order + Q_BLOCK], axis=2).reshape(SEQS, 2 * Q_BLOCK)
    route_ids = jnp.take_along_axis(owner, pick, axis=1).reshape(TOKENS, 2)
    route_slots = jnp.take_along_axis(rank, pick, axis=1).reshape(TOKENS, 2)
    return (route_ids.astype(jnp.int32), route_slots.astype(jnp.int32))


def draw_route_ids(key, part):
    return route_table(key)[0]


def draw_route_slots(key, part):
    return route_table(key)[1]


def draw_route_weights(key, part):
    leading = jax.random.randint(jax.random.fold_in(key, 3), (TOKENS,), 1, 65536)
    return jnp.stack([leading, 65536 - leading], axis=1).astype(jnp.int32)


def levels(stream_key, shape, shards, least, top_value):
    loudness, own = 1.0, jax.random.fold_in(stream_key, 6)
    for axis_at, parts in shards:
        heights = jnp.exp(jax.random.uniform(jax.random.fold_in(own, axis_at), (parts,), jnp.float32, least / len(shards), top_value / len(shards)))
        loudness = loudness * jnp.repeat(heights, shape[axis_at] // parts).reshape([-1 if axis == axis_at else 1 for axis in range(len(shape))])
    return loudness


def normal_values(rng, extent, scale, bound, pieces=(), kind=jnp.bfloat16):
    factor_of = levels(rng, extent, pieces, -0.22, 0.18) if pieces else 1.0
    entries = jax.random.normal(rng, extent, jnp.float32) * scale * factor_of
    return jnp.minimum(jnp.maximum(entries, -bound), bound).astype(kind)


def setup_inputs(seed: int = 0, part: int = 0) -> dict:
    key_list = jax.random.split(jax.random.key(seed), 13)
    part_keys = jax.random.split(jax.random.fold_in(key_list[12], part), 13)
    return {
        "queries": draw_queries(jax.random.fold_in(jax.random.fold_in(key_list[12], part), 71), part),
        "keys": draw_keys(jax.random.fold_in(jax.random.fold_in(key_list[12], part), 71), part),
        "values": normal_values(part_keys[2], (SEQS, CTX, KV_HEADS * HEAD_DIM), 1.0, 4.0, ((0, 32), (2, 4))),
        "out_weight": normal_values(key_list[3], (HEADS * HEAD_DIM, D), HEAD_DIM ** -0.5, 0.5, ((0, 4), (1, 32))),
        "residual": normal_values(part_keys[4], (TOKENS, D), 0.5, 3.0, ((0, 32),)),
        "norm_gain": jnp.clip(1.0 + 0.1 * jax.random.normal(key_list[5], (D,), jnp.float32), 0.5, 1.5),
        "route_ids": draw_route_ids(jax.random.fold_in(jax.random.fold_in(key_list[12], part), 71), part),
        "route_slots": draw_route_slots(jax.random.fold_in(jax.random.fold_in(key_list[12], part), 71), part),
        "route_weights": draw_route_weights(jax.random.fold_in(jax.random.fold_in(key_list[12], part), 71), part),
        "w_gate": normal_values(key_list[9], (EXPERTS, D, FFW), D ** -0.5, 0.09375, ((0, 4), (2, 32))),
        "w_up": normal_values(key_list[10], (EXPERTS, D, FFW), D ** -0.5, 0.09375, ((0, 4), (2, 32))),
        "w_down": normal_values(key_list[11], (EXPERTS, FFW, D), FFW ** -0.5, 0.0625, ((0, 4), (1, 32))),
    }


eps = 1e-05

def attend_one(item):
    query_block, key_block, value_block = item
    block = query_block.shape[0]
    context = key_block.shape[0]
    group = HEADS // KV_HEADS
    query_heads = query_block.reshape(block, KV_HEADS, group, HEAD_DIM).astype(jnp.float32)
    key_heads = key_block.reshape(context, KV_HEADS, HEAD_DIM).astype(jnp.float32)
    value_heads = value_block.reshape(context, KV_HEADS, HEAD_DIM).astype(jnp.float32)
    scores = jnp.einsum('qcgd,kcd->cgqk', query_heads, key_heads) * HEAD_DIM ** (-0.5)
    key_pos = jnp.arange(context)
    query_pos = context - block + jnp.arange(block)
    allowed = key_pos[None, :] <= query_pos[:, None]
    masked = jnp.where(allowed, scores, -1e+30)
    highest = lax.optimization_barrier(jnp.max(masked, axis=-1, keepdims=True))
    weights = jnp.where(allowed, jnp.exp(masked - highest), 0.0)
    probs = (weights / lax.optimization_barrier(jnp.sum(weights, axis=-1, keepdims=True))).astype(jnp.bfloat16)
    heads_out = jnp.einsum('cgqk,kcd->qcgd', probs.astype(jnp.float32), value_heads)
    return heads_out.astype(jnp.bfloat16).reshape(block, HEADS * HEAD_DIM)

def expert_one(item):
    rows, gate_w, up_w, down_w = item
    gate = jnp.dot(rows, gate_w, preferred_element_type=jnp.float32)
    upper = jnp.dot(rows, up_w, preferred_element_type=jnp.float32)
    hidden = (jax.nn.silu(gate) * upper).astype(jnp.bfloat16)
    width = FFW // N_FSDP
    hidden_runs = hidden.reshape(rows.shape[0], N_FSDP, width).transpose(1, 0, 2)
    down_runs = down_w.reshape(N_FSDP, width, down_w.shape[1])

    def add_run(total, pair):
        part = jnp.dot(pair[0], pair[1], preferred_element_type=jnp.float32)
        part = lax.optimization_barrier(part.astype(jnp.bfloat16)).astype(jnp.float32)
        return (total + part, None)
    start_total = jnp.zeros((rows.shape[0], down_w.shape[1]), jnp.float32)
    total, unused = lax.scan(add_run, start_total, (hidden_runs, down_runs))
    return total

def reference(queries, keys, values, out_weight, residual, norm_gain, route_ids, route_slots, route_weights, w_gate, w_up, w_down):
    query_blocks = queries.reshape(SEQS, Q_BLOCK, HEADS * HEAD_DIM)
    heads_out = lax.map(attend_one, (query_blocks, keys, values)).reshape(TOKENS, HEADS * HEAD_DIM)
    attn = jnp.dot(heads_out, out_weight, preferred_element_type=jnp.float32)
    hstate = (residual.astype(jnp.float32) + attn).astype(jnp.bfloat16)
    state = hstate.astype(jnp.float32)
    scale = lax.rsqrt(lax.optimization_barrier(jnp.mean(state * state, axis=-1, keepdims=True)) + eps)
    normed = (state * scale * norm_gain).astype(jnp.bfloat16)
    block_of = (jnp.arange(TOKENS) // Q_BLOCK).astype(jnp.int32)
    spread = jnp.broadcast_to(normed[:, None, :], (TOKENS, 2, D))
    buffer = jnp.zeros((SEQS, EXPERTS, CAP, D), jnp.bfloat16)
    buffer = buffer.at[block_of[:, None], route_ids, route_slots].set(spread)
    expert_rows = buffer.transpose(1, 0, 2, 3).reshape(EXPERTS, SEQS * CAP, D)
    expert_out = lax.map(expert_one, (expert_rows, w_gate, w_up, w_down)).reshape(EXPERTS, SEQS, CAP, D)
    picked = expert_out[route_ids, block_of[:, None], route_slots]
    route_share = route_weights.astype(jnp.float32) / 65536.0
    moe = lax.optimization_barrier(jnp.sum(route_share[:, :, None] * picked, axis=1))
    return (hstate.astype(jnp.float32) + moe).astype(jnp.bfloat16)
```

```python
import functools

import jax
import jax.numpy as jnp
from jax import lax
from jax.experimental import pallas as pl
from jax.experimental.pallas import tpu as pltpu
from jax.sharding import PartitionSpec as P

HEAD_DIM = 128
GCAP = 36
SUBS = 4
EPS = 1e-05
MESH = pl.DeviceIdType.MESH
F32 = jnp.float32
BF16 = jnp.bfloat16


def dot(a, b):
    return jnp.dot(a, b, preferred_element_type=F32)


def layer_kernel(
    nz,
    q_ref,
    k_hbm,
    v_hbm,
    ow_hbm,
    res_hbm,
    gain_ref,
    ids_ref,
    slots_ref,
    weights_ref,
    wg_hbm,
    wu_hbm,
    wd_hbm,
    out_ref,
    keys,
    vals,
    res,
    wg,
    wu,
    wd,
    heads,
    ow,
    xa,
    xar,
    xb,
    xbr,
    hst,
    own,
    oth,
    rows,
    cnt,
    acc,
    hid,
    part,
    dbuf,
    rbuf,
    fin,
    finr,
    con,
    conr,
    lsem,
    d0_s,
    d0_r,
    r1_s,
    r1_r,
    d1_s,
    d1_r,
    xa_s,
    xa_r,
    xb_s,
    xb_r,
    ot_s,
    ot_r,
    r2_s,
    r2_r,
    d2_s,
    d2_r,
    c0_s,
    c0_r,
    cr_s,
    cr_r,
    cd_s,
    cd_r,
    db_s,
    db_r,
    rs_s,
    rs_r,
    fi_s,
    fi_r,
    co_s,
    co_r,
):
    half = nz // 2
    n2 = lax.axis_index("fsdp")
    c = lax.rem(n2, 2)
    z = n2 // 2
    x = lax.axis_index("expert")
    step_dir = 2 * c - 1
    ring_next = {"fsdp": lax.rem(z + step_dir + nz, nz) * 2 + c}
    ring_prev = {"fsdp": lax.rem(z - step_dir + nz, nz) * 2 + c}
    sibling = {"fsdp": z * 2 + 1 - c}
    x_first = {"expert": x + 1 - 2 * lax.rem(x, 2)}
    x_second = {"expert": 3 - x}
    x_other = [{"expert": lax.rem(x + o, 4)} for o in range(4)]

    def unit_at(s):
        return lax.rem(z + s * step_dir + 2 * nz, nz)

    def sub_at(k):
        return lax.rem(2 * c + k, SUBS)

    def send(src, dst, s_sem, r_sem, device):
        return pltpu.make_async_remote_copy(
            src_ref=src, dst_ref=dst, send_sem=s_sem, recv_sem=r_sem,
            device_id=device, device_id_type=MESH,
        )

    def ring1(s, j, u):
        ref = ow.at[u, j]
        return send(ref, ref, r1_s.at[s, j], r1_r.at[s, j], ring_next)

    def pair1(s, j, u):
        ref = ow.at[u, j]
        return send(ref, ref, d1_s.at[s, j], d1_r.at[s, j], sibling)

    def ring2(s, j, u):
        ref = rows.at[u, j]
        return send(ref, ref, r2_s.at[s, j], r2_r.at[s, j], ring_next)

    def pair2(s, j, u):
        ref = rows.at[u, j]
        return send(ref, ref, d2_s.at[s, j], d2_r.at[s, j], sibling)

    def count_ring(s, u):
        return send(cnt.at[u], cnt.at[u], cr_s.at[s], cr_r.at[s], ring_next)

    def count_pair(s, u):
        return send(cnt.at[u], cnt.at[u], cd_s.at[s], cd_r.at[s], sibling)

    def swap_a(s):
        return send(xa.at[s], xar.at[s], xa_s.at[s], xa_r.at[s], x_first)

    def swap_b(s):
        return send(xb.at[s], xbr.at[s], xb_s.at[s], xb_r.at[s], x_second)

    def give(s, j, u):
        return send(part.at[u, j], dbuf.at[s - 1, j], db_s.at[s - 1, j], db_r.at[s - 1, j], sibling)

    def ring3(t, j, u):
        return send(part.at[u, j], rbuf.at[t - 1, j], rs_s.at[t - 1, j], rs_r.at[t - 1, j], ring_next)

    own_rows = ow_hbm.shape[0] // 2
    loads = [
        pltpu.make_async_copy(ow_hbm.at[pl.ds(0, own_rows)], ow.at[z, 2 * c], lsem.at[0]),
        pltpu.make_async_copy(ow_hbm.at[pl.ds(own_rows, own_rows)], ow.at[z, 2 * c + 1], lsem.at[1]),
        pltpu.make_async_copy(k_hbm.at[0], keys, lsem.at[2]),
        pltpu.make_async_copy(v_hbm.at[0], vals, lsem.at[3]),
        pltpu.make_async_copy(res_hbm, res, lsem.at[4]),
        pltpu.make_async_copy(wg_hbm, wg, lsem.at[5]),
        pltpu.make_async_copy(wu_hbm, wu, lsem.at[6]),
        pltpu.make_async_copy(wd_hbm, wd, lsem.at[7]),
    ]
    for load in loads:
        load.start()

    barrier = pltpu.get_barrier_semaphore()
    partners = [ring_next, ring_prev, sibling, *x_other[1:]]
    for device in partners:
        pl.semaphore_signal(barrier, inc=1, device_id=device, device_id_type=MESH)
    pl.semaphore_wait(barrier, len(partners))

    loads[0].wait()
    loads[1].wait()
    for i in range(2):
        j = 2 * c + i
        send(ow.at[z, j], ow.at[z, j], d0_s.at[i], d0_r.at[i], sibling).start()
        ring1(1, j, z).start()
    for i in range(2):
        j = 2 * (1 - c) + i
        send(ow.at[z, j], ow.at[z, j], d0_s.at[i], d0_r.at[i], sibling).wait_recv()
        ring1(1, j, z).start()

    loads[2].wait()
    loads[3].wait()
    block, heads_width = q_ref.shape
    context = keys.shape[0]
    key_pos = lax.broadcasted_iota(jnp.int32, (block, context), 1)
    query_pos = context - block + lax.broadcasted_iota(jnp.int32, (block, context), 0)
    allowed = key_pos <= query_pos
    for h in range(heads_width // HEAD_DIM):
        cols = slice(h * HEAD_DIM, (h + 1) * HEAD_DIM)
        scores = lax.dot_general(
            q_ref[:, cols], keys[...], (((1,), (1,)), ((), ())), preferred_element_type=F32
        ) * HEAD_DIM ** (-0.5)
        masked = jnp.where(allowed, scores, -1e30)
        highest = jnp.max(masked, axis=-1, keepdims=True)
        weights = jnp.where(allowed, jnp.exp(masked - highest), 0.0)
        probs = (weights / jnp.sum(weights, axis=-1, keepdims=True)).astype(BF16)
        heads[:, cols] = dot(probs, vals[...]).astype(BF16)

    unit = 2 * ow.shape[3]
    lane = ow.shape[3]

    def project(s):
        for pos, u in enumerate((unit_at(-s), unit_at(s))):
            for b in range(2):
                total = dot(heads[:, :own_rows], ow[u, 2 * b]) + dot(
                    heads[:, own_rows:], ow[u, 2 * b + 1]
                )
                at = pos * unit + b * lane
                xa[s, :, at : at + lane] = total.astype(BF16)
        swap_a(s).start()

    def add_first(s):
        swap_a(s).wait_recv()
        xb[s] = (xa[s].astype(F32) + xar[s].astype(F32)).astype(BF16)
        swap_b(s).start()

    def add_second(s):
        swap_b(s).wait_recv()
        for pos, u in enumerate((unit_at(-s), unit_at(s))):
            cols = slice(pos * unit, (pos + 1) * unit)
            attn = xb[s, :, cols].astype(F32) + xbr[s, :, cols].astype(F32)
            left = pl.ds(pl.multiple_of(u * unit, unit), unit)
            hst[u] = (res[:, left].astype(F32) + attn).astype(BF16)

    loads[4].wait()
    project(0)

    def projection_step(s, carry):
        u = unit_at(-s)
        for k in range(SUBS):
            j = sub_at(k)
            ring1(s, j, u).wait_recv()
            if k < 2:
                ring1(s + 1, j, u).start()
            else:
                @pl.when(s < half - 1)
                def _():
                    ring1(s + 1, j, u).start()
            pair1(s, j, u).start()
        for j in range(SUBS):
            pair1(s, j, unit_at(s)).wait_recv()
        project(s)
        add_first(s - 1)

        @pl.when(s >= 2)
        def _():
            add_second(s - 2)

        return carry

    lax.fori_loop(1, half, projection_step, 0)
    u = unit_at(half)
    for k in range(2):
        j = sub_at(k)
        ring1(half, j, u).wait_recv()
        pair1(half, j, u).start()
    for k in range(2, 4):
        pair1(half, sub_at(k), u).wait_recv()
    project(half)
    add_first(half - 1)
    add_second(half - 2)
    add_first(half)
    add_second(half - 1)
    add_second(half)

    width = rows.shape[3]
    per_sub = width // unit
    d_model = width * SUBS
    square = jnp.zeros((block, 1), F32)
    for i in range(nz):
        state = hst[i].astype(F32)
        square = square + jnp.sum(state * state, axis=-1, keepdims=True)
    scale = lax.rsqrt(square / d_model + EPS)
    first_expert = 2 * x
    ids = ids_ref[...]
    within = ids - first_expert
    in_group = (within >= 0) & (within < 2)
    is_first = jnp.where(ids == first_expert, 1.0, 0.0)
    lead = jnp.sum(jnp.sum(is_first, axis=1, keepdims=True), axis=0, keepdims=True)
    lead_i = lead.astype(jnp.int32)
    target = jnp.where(in_group, slots_ref[...] + within * lead_i + GCAP * c, -1)
    row_ids = lax.broadcasted_iota(jnp.int32, (block, 2 * GCAP), 1)
    picks = [(target[:, k : k + 1] == row_ids) for k in range(2)]
    one_hot = jnp.where(picks[0] | picks[1], 1.0, 0.0).astype(BF16)
    cnt[z, c] = jnp.broadcast_to(lead, cnt.shape[2:])
    to_sibling = send(cnt.at[z, c], cnt.at[z, c], c0_s.at[0], c0_r.at[0], sibling)
    to_sibling.start()
    for k in range(SUBS):
        j = sub_at(k)
        for i in range(per_sub):
            u = j * per_sub + i
            gain = gain_ref[:, pl.ds(pl.multiple_of(u * unit, unit), unit)]
            normed = (hst[u].astype(F32) * scale * gain).astype(BF16)
            own[j, :, i * unit : (i + 1) * unit] = lax.dot_general(
                one_hot, normed, (((0,), (0,)), ((), ())), preferred_element_type=F32
            ).astype(BF16)
        send(own.at[j], oth.at[j], ot_s.at[j], ot_r.at[j], sibling).start()
    send(cnt.at[z, 1 - c], cnt.at[z, 1 - c], c0_s.at[0], c0_r.at[0], sibling).wait_recv()
    count_ring(1, z).start()
    for k in range(SUBS):
        j = sub_at(k)
        send(own.at[j], oth.at[j], ot_s.at[j], ot_r.at[j], sibling).wait_recv()
        rows[z, j] = own[j] + oth[j]
        ring2(1, j, z).start()

    for load in loads[5:]:
        load.wait()
    unit_rows = 2 * GCAP
    ffw = wg.shape[2]

    def arrive_count(s, last):
        u = unit_at(-s)
        count_ring(s, u).wait_recv()
        if not last:
            count_ring(s + 1, u).start()
            count_pair(s, u).start()

    def gate_up(s, k, places):
        j = sub_at(k)
        slab = pl.ds(pl.multiple_of(j * width, width), width)
        for pos, u in places:
            block_rows = rows[u, j]
            for e in range(2):
                g = dot(block_rows, wg[e, slab, :])
                up = dot(block_rows, wu[e, slab, :])
                if k == 0:
                    acc[pos, e] = g
                    acc[pos, 2 + e] = up
                else:
                    acc[pos, e] += g
                    acc[pos, 2 + e] += up

    def activate(s, places):
        row = lax.broadcasted_iota(jnp.int32, (unit_rows, ffw), 0).astype(F32)
        upper = row >= GCAP
        place = jnp.where(upper, row - GCAP, row)
        for pos, u in places:
            limit = jnp.where(upper, cnt[u, 1, 0:1, 0:1], cnt[u, 0, 0:1, 0:1])
            second = place >= limit
            for e in range(2):
                g, up = acc[pos, e], acc[pos, 2 + e]
                value = g / (1.0 + jnp.exp(-g)) * up
                mine = second if e == 1 else jnp.logical_not(second)
                hid[lax.rem(s, 2), pos, e] = jnp.where(mine, value, 0.0).astype(BF16)

    def down(s, k, places):
        j = sub_at(k)
        cols = pl.ds(pl.multiple_of(j * width, width), width)
        for pos, u in places:
            total = dot(hid[lax.rem(s, 2), pos, 0], wd[0, :, cols])
            total = total + dot(hid[lax.rem(s, 2), pos, 1], wd[1, :, cols])
            part[u, j] = total.astype(BF16)

    def both(s):
        return ((0, unit_at(-s)), (1, unit_at(s)))

    def expert_step(s, carry):
        arrive_count(s, False)
        u = unit_at(-s)
        for k in range(SUBS):
            j = sub_at(k)
            ring2(s, j, u).wait_recv()
            if k < 2:
                ring2(s + 1, j, u).start()
            else:
                @pl.when(s < half - 1)
                def _():
                    ring2(s + 1, j, u).start()
            pair2(s, j, u).start()

            @pl.when(s >= 2)
            def _():
                pair2(s - 1, j, unit_at(s - 1)).wait_recv()

            gate_up(s - 1, k, both(s - 1))
            if k == SUBS - 1:
                @pl.when(s >= 2)
                def _():
                    count_pair(s - 1, unit_at(s - 1)).wait_recv()

                activate(s - 1, both(s - 1))

            @pl.when(s >= 2)
            def _():
                down(s - 2, k, both(s - 2))

            @pl.when(s >= 3)
            def _():
                give(s - 2, j, unit_at(2 - s)).start()

        return carry

    lax.fori_loop(1, half, expert_step, 0)

    far = unit_at(half)
    arrive_count(half, True)
    for k in range(SUBS):
        j = sub_at(k)
        if k < 2:
            ring2(half, j, far).wait_recv()
            pair2(half, j, far).start()
        pair2(half - 1, j, unit_at(half - 1)).wait_recv()
        gate_up(half - 1, k, both(half - 1))
        down(half - 2, k, both(half - 2))
        if half - 2 >= 1:
            give(half - 2, j, unit_at(2 - half)).start()
    count_pair(half - 1, unit_at(half - 1)).wait_recv()
    activate(half - 1, both(half - 1))
    single = ((0, far),)
    for k in range(SUBS):
        if k >= 2:
            pair2(half, sub_at(k), far).wait_recv()
        gate_up(half, k, single)
    activate(half, single)
    for k in (2, 3, 0, 1):
        down(half, k, single)
        if k >= 2:
            give(half, sub_at(k), far).start()

    for k in range(2):
        j = sub_at(k)
        give(half, j, far).wait_recv()
        part[far, j] = (part[far, j].astype(F32) + dbuf[half - 1, j].astype(F32)).astype(BF16)
        ring3(1, j, far).start()
    for k in range(SUBS):
        j = sub_at(k)
        down(half - 1, k, both(half - 1))
        give(half - 1, j, unit_at(1 - half)).start()

    def sum_sub(t, k, arrived):
        j = sub_at(k)
        u = unit_at(half - t)
        give(half - t, j, u).wait_recv()
        total = part[u, j].astype(F32) + dbuf[half - t - 1, j].astype(F32)
        if arrived:
            ring3(t, j, u).wait_recv()
            total = total + rbuf[t - 1, j].astype(F32)
        part[u, j] = total.astype(BF16)
        ring3(t + 1, j, u).start()

    for k in (2, 3, 0, 1):
        sum_sub(1, k, k < 2)

    def sum_step(t, carry):
        for k in range(SUBS):
            sum_sub(t, (k + 2) % SUBS, True)
        return carry

    lax.fori_loop(2, half, sum_step, 0)

    def finish(j):
        return send(fin.at[j], finr.at[j], fi_s.at[j], fi_r.at[j], sibling)

    for k in (2, 3, 0, 1):
        j = sub_at(k)
        ring3(half, j, z).wait_recv()
        fin[j] = (part[z, j].astype(F32) + rbuf[half - 1, j].astype(F32)).astype(BF16)
        finish(j).start()

    share = jnp.where(in_group, weights_ref[...].astype(F32) / 65536.0, 0.0)
    chosen = [jnp.where(pick, 1.0, 0.0).astype(BF16) for pick in picks]

    def combine(j):
        finish(j).wait_recv()
        total = (fin[j].astype(F32) + finr[j].astype(F32)).astype(BF16)
        return share[:, 0:1] * dot(chosen[0], total) + share[:, 1:2] * dot(chosen[1], total)

    def deliver(o):
        return send(con.at[o - 1], conr.at[o - 1], co_s.at[o - 1], co_r.at[o - 1], x_other[o])

    for o in (2, 1, 3):
        con[o - 1] = combine(lax.rem(x + o, 4)).astype(BF16)
        deliver(o).start()
    mine = combine(x)
    for i in range(per_sub):
        cols = slice(i * unit, (i + 1) * unit)
        out_ref[:, cols] = hst[x * per_sub + i].astype(BF16)
    for o in (1, 3, 2):
        deliver(o).wait_recv()
    moe = mine + conr[0].astype(F32) + conr[1].astype(F32) + conr[2].astype(F32)
    out_ref[...] = (out_ref[...].astype(F32) + moe).astype(BF16)

    for i in range(2):
        send(ow.at[z, i], ow.at[z, i], d0_s.at[i], d0_r.at[i], sibling).wait_send()
    to_sibling.wait_send()

    def drain(s, carry):
        count_ring(s, z).wait_send()
        swap_a(s - 1).wait_send()
        swap_b(s - 1).wait_send()
        for j in range(SUBS):
            @pl.when(s < half)
            def _():
                for make in (ring1, ring2, pair1, pair2, give):
                    make(s, j, z).wait_send()
                ring3(s + 1, j, z).wait_send()

        @pl.when(s < half)
        def _():
            count_pair(s, z).wait_send()

        return carry

    lax.fori_loop(1, half + 1, drain, 0)
    swap_a(half).wait_send()
    swap_b(half).wait_send()
    for k in range(2):
        j = sub_at(k)
        for make in (ring1, ring2, pair1, pair2):
            make(half, j, z).wait_send()
        give(half, sub_at(k + 2), z).wait_send()
        ring3(1, j, z).wait_send()
    for j in range(SUBS):
        send(own.at[j], oth.at[j], ot_s.at[j], ot_r.at[j], sibling).wait_send()
        finish(j).wait_send()
    for o in (1, 2, 3):
        deliver(o).wait_send()


def per_device(nz, *args):
    (queries, keys, values, out_weight, residual, gain, ids, slots, weights, w_gate, w_up, w_down) = args
    block, heads_width = queries.shape
    d_model = residual.shape[1]
    width = d_model // SUBS
    half = nz // 2
    lane = out_weight.shape[1]
    ow_rows = out_weight.shape[0] // 2
    unit_rows = 2 * GCAP
    ffw = w_gate.shape[2]
    vmem = pl.BlockSpec(memory_space=pltpu.VMEM)
    hbm = pl.BlockSpec(memory_space=pl.ANY)
    dma = pltpu.SemaphoreType.DMA
    swap = pltpu.VMEM((half + 1, block, 4 * lane), BF16)
    sub = pltpu.VMEM((SUBS, unit_rows, width), BF16)
    scratch = [
        pltpu.VMEM(keys.shape[1:], BF16),
        pltpu.VMEM(values.shape[1:], BF16),
        pltpu.VMEM(residual.shape, BF16),
        pltpu.VMEM(w_gate.shape, BF16),
        pltpu.VMEM(w_up.shape, BF16),
        pltpu.VMEM(w_down.shape, BF16),
        pltpu.VMEM((block, heads_width), BF16),
        pltpu.VMEM((nz, SUBS, ow_rows, lane), BF16),
        swap,
        swap,
        swap,
        swap,
        pltpu.VMEM((nz, block, 2 * lane), BF16),
        sub,
        sub,
        pltpu.VMEM((nz, SUBS, unit_rows, width), BF16),
        pltpu.VMEM((nz, 2, 8, 128), F32),
        pltpu.VMEM((2, 4, unit_rows, ffw), F32),
        pltpu.VMEM((2, 2, 2, unit_rows, ffw), BF16),
        pltpu.VMEM((nz, SUBS, unit_rows, width), BF16),
        pltpu.VMEM((half, SUBS, unit_rows, width), BF16),
        pltpu.VMEM((half, SUBS, unit_rows, width), BF16),
        sub,
        sub,
        pltpu.VMEM((3, block, width), BF16),
        pltpu.VMEM((3, block, width), BF16),
        dma((8,)),
        dma((2,)),
        dma((2,)),
        *[dma((half + 1, SUBS))] * 4,
        *[dma((half + 1,))] * 4,
        *[dma((SUBS,))] * 2,
        *[dma((half + 1, SUBS))] * 4,
        *[dma((1,))] * 2,
        *[dma((half + 1,))] * 4,
        *[dma((half, SUBS))] * 4,
        *[dma((SUBS,))] * 2,
        *[dma((3,))] * 2,
    ]
    return pl.pallas_call(
        functools.partial(layer_kernel, nz),
        out_shape=jax.ShapeDtypeStruct((block, width), BF16),
        in_specs=[vmem, hbm, hbm, hbm, hbm, vmem, vmem, vmem, vmem, hbm, hbm, hbm],
        out_specs=vmem,
        scratch_shapes=scratch,
        compiler_params=pltpu.CompilerParams(
            collective_id=0, has_side_effects=True, vmem_limit_bytes=67043328
        ),
    )(queries, keys, values, out_weight, residual, gain.reshape(1, -1), ids, slots, weights, w_gate, w_up, w_down)


def solution(mesh):
    in_specs = (
        P(("groups", "fsdp"), "expert"),
        P(("groups", "fsdp"), None, "expert"),
        P(("groups", "fsdp"), None, "expert"),
        P("expert", "fsdp"),
        P(("groups", "fsdp"), None),
        P(),
        P(("groups", "fsdp"), None),
        P(("groups", "fsdp"), None),
        P(("groups", "fsdp"), None),
        P("expert", None, "fsdp"),
        P("expert", None, "fsdp"),
        P("expert", "fsdp", None),
    )
    return jax.shard_map(
        functools.partial(per_device, mesh.shape["fsdp"] // 2),
        mesh=mesh,
        in_specs=in_specs,
        out_specs=P(("groups", "fsdp"), "expert"),
        check_vma=False,
    )
```

```python
import functools

import jax
import jax.numpy as jnp
from jax import lax
from jax.experimental import pallas as pl
from jax.experimental.pallas import tpu as pltpu
from jax.sharding import PartitionSpec as P

HEAD_DIM = 128
GCAP = 36
SUBS = 4
EPS = 1e-05
MESH = pl.DeviceIdType.MESH
F32 = jnp.float32
BF16 = jnp.bfloat16


def dot(a, b):
    return jnp.dot(a, b, preferred_element_type=F32)


def layer_kernel(
    nz,
    q_ref,
    k_hbm,
    v_hbm,
    ow_hbm,
    res_hbm,
    gain_ref,
    ids_ref,
    slots_ref,
    weights_ref,
    wg_hbm,
    wu_hbm,
    wd_hbm,
    out_ref,
    keys,
    vals,
    res,
    wg,
    wu,
    wd,
    heads,
    ow,
    xa,
    xar,
    xb,
    xbr,
    hst,
    own,
    oth,
    rows,
    cnt,
    acc,
    hid,
    part,
    dbuf,
    rbuf,
    fin,
    finr,
    con,
    conr,
    own_out,
    xh,
    xhr,
    mix,
    lsem,
    d0_s,
    d0_r,
    r1_s,
    r1_r,
    d1_s,
    d1_r,
    xa_s,
    xa_r,
    xb_s,
    xb_r,
    ot_s,
    ot_r,
    r2_s,
    r2_r,
    d2_s,
    d2_r,
    c0_s,
    c0_r,
    cr_s,
    cr_r,
    cd_s,
    cd_r,
    db_s,
    db_r,
    rs_s,
    rs_r,
    fi_s,
    fi_r,
    co_s,
    co_r,
    xh_s,
    xh_r,
):
    half = nz // 2
    n2 = lax.axis_index("fsdp")
    c = lax.rem(n2, 2)
    z = n2 // 2
    x = lax.axis_index("expert")
    step_dir = 2 * c - 1
    ring_next = {"fsdp": lax.rem(z + step_dir + nz, nz) * 2 + c}
    ring_prev = {"fsdp": lax.rem(z - step_dir + nz, nz) * 2 + c}
    sibling = {"fsdp": z * 2 + 1 - c}
    x_first = {"expert": x + 1 - 2 * lax.rem(x, 2)}
    x_second = {"expert": 3 - x}
    x_other = [{"expert": lax.rem(x + o, 4)} for o in range(4)]

    def unit_at(s):
        return lax.rem(z + s * step_dir + 2 * nz, nz)

    def sub_at(k):
        return lax.rem(2 * c + k, SUBS)

    def send(src, dst, s_sem, r_sem, device):
        return pltpu.make_async_remote_copy(
            src_ref=src, dst_ref=dst, send_sem=s_sem, recv_sem=r_sem,
            device_id=device, device_id_type=MESH,
        )

    def ring1(s, j, u):
        ref = ow.at[u, j]
        return send(ref, ref, r1_s.at[s, j], r1_r.at[s, j], ring_next)

    def pair1(s, j, u):
        ref = ow.at[u, j]
        return send(ref, ref, d1_s.at[s, j], d1_r.at[s, j], sibling)

    def ring2(s, j, u):
        ref = rows.at[u, j]
        return send(ref, ref, r2_s.at[s, j], r2_r.at[s, j], ring_next)

    def pair2(s, j, u):
        ref = rows.at[u, j]
        return send(ref, ref, d2_s.at[s, j], d2_r.at[s, j], sibling)

    def count_ring(s, u):
        return send(cnt.at[u], cnt.at[u], cr_s.at[s], cr_r.at[s], ring_next)

    def count_pair(s, u):
        return send(cnt.at[u], cnt.at[u], cd_s.at[s], cd_r.at[s], sibling)

    def swap_a(s):
        return send(xa.at[s], xar.at[s], xa_s.at[s], xa_r.at[s], x_first)

    def swap_b(s):
        return send(xb.at[s], xbr.at[s], xb_s.at[s], xb_r.at[s], x_second)

    def give(s, j, u):
        return send(part.at[u, j], dbuf.at[s - 1, j], db_s.at[s - 1, j], db_r.at[s - 1, j], sibling)

    def ring3(t, j, u):
        return send(part.at[u, j], rbuf.at[t - 1, j], rs_s.at[t - 1, j], rs_r.at[t - 1, j], ring_next)

    own_rows = ow_hbm.shape[0] // 2
    loads = [
        pltpu.make_async_copy(ow_hbm.at[pl.ds(0, own_rows)], ow.at[z, 2 * c], lsem.at[0]),
        pltpu.make_async_copy(ow_hbm.at[pl.ds(own_rows, own_rows)], ow.at[z, 2 * c + 1], lsem.at[1]),
        pltpu.make_async_copy(k_hbm.at[0], keys, lsem.at[2]),
        pltpu.make_async_copy(v_hbm.at[0], vals, lsem.at[3]),
        pltpu.make_async_copy(res_hbm, res, lsem.at[4]),
        pltpu.make_async_copy(wg_hbm, wg, lsem.at[5]),
        pltpu.make_async_copy(wu_hbm, wu, lsem.at[6]),
        pltpu.make_async_copy(wd_hbm, wd, lsem.at[7]),
    ]
    for load in loads:
        load.start()

    barrier = pltpu.get_barrier_semaphore()
    partners = [ring_next, ring_prev, sibling, *x_other[1:]]
    for device in partners:
        pl.semaphore_signal(barrier, inc=1, device_id=device, device_id_type=MESH)
    pl.semaphore_wait(barrier, len(partners))

    loads[0].wait()
    loads[1].wait()
    for i in range(2):
        j = 2 * c + i
        send(ow.at[z, j], ow.at[z, j], d0_s.at[i], d0_r.at[i], sibling).start()
        ring1(1, j, z).start()
    for i in range(2):
        j = 2 * (1 - c) + i
        send(ow.at[z, j], ow.at[z, j], d0_s.at[i], d0_r.at[i], sibling).wait_recv()
        ring1(1, j, z).start()

    loads[2].wait()
    loads[3].wait()
    block, heads_width = q_ref.shape
    context = keys.shape[0]
    key_pos = lax.broadcasted_iota(jnp.int32, (block, context), 1)
    query_pos = context - block + lax.broadcasted_iota(jnp.int32, (block, context), 0)
    allowed = key_pos <= query_pos
    for h in range(heads_width // HEAD_DIM):
        cols = slice(h * HEAD_DIM, (h + 1) * HEAD_DIM)
        scores = lax.dot_general(
            q_ref[:, cols], keys[...], (((1,), (1,)), ((), ())), preferred_element_type=F32
        ) * HEAD_DIM ** (-0.5)
        masked = jnp.where(allowed, scores, -1e30)
        highest = jnp.max(masked, axis=-1, keepdims=True)
        weights = jnp.where(allowed, jnp.exp(masked - highest), 0.0)
        probs = (weights / jnp.sum(weights, axis=-1, keepdims=True)).astype(BF16)
        heads[:, cols] = dot(probs, vals[...]).astype(BF16)

    unit = 2 * ow.shape[3]
    lane = ow.shape[3]

    def project(s):
        for pos, u in enumerate((unit_at(-s), unit_at(s))):
            for b in range(2):
                total = dot(heads[:, :own_rows], ow[u, 2 * b]) + dot(
                    heads[:, own_rows:], ow[u, 2 * b + 1]
                )
                at = pos * unit + b * lane
                xa[s, :, at : at + lane] = total.astype(BF16)
        swap_a(s).start()

    def add_first(s):
        swap_a(s).wait_recv()
        xb[s] = (xa[s].astype(F32) + xar[s].astype(F32)).astype(BF16)
        swap_b(s).start()

    def add_second(s):
        swap_b(s).wait_recv()
        for pos, u in enumerate((unit_at(-s), unit_at(s))):
            cols = slice(pos * unit, (pos + 1) * unit)
            attn = xb[s, :, cols].astype(F32) + xbr[s, :, cols].astype(F32)
            left = pl.ds(pl.multiple_of(u * unit, unit), unit)
            hst[u] = (res[:, left].astype(F32) + attn).astype(BF16)

    loads[4].wait()

    def take_pair(s):
        for j in range(SUBS):
            pair1(s, j, unit_at(s)).wait_recv()

    def projection_step(s, carry):
        u = unit_at(-s)
        for k in range(SUBS):
            j = sub_at(k)
            ring1(s, j, u).wait_recv()
            if k < 2:
                ring1(s + 1, j, u).start()
            else:
                @pl.when(s < half - 1)
                def _():
                    ring1(s + 1, j, u).start()
            pair1(s, j, u).start()
        @pl.when(s >= 2)
        def _():
            take_pair(s - 1)

        project(s - 1)
        @pl.when(s >= 2)
        def _():
            add_first(s - 2)

        @pl.when(s >= 3)
        def _():
            add_second(s - 3)

        return carry

    lax.fori_loop(1, half, projection_step, 0)
    u = unit_at(half)
    ring1(half, sub_at(0), u).wait_recv()
    pair1(half, sub_at(0), u).start()
    take_pair(half - 1)
    project(half - 1)
    ring1(half, sub_at(1), u).wait_recv()
    pair1(half, sub_at(1), u).start()
    add_first(half - 2)
    if half >= 3:
        add_second(half - 3)
    for k in range(2, 4):
        pair1(half, sub_at(k), u).wait_recv()
    for b in range(2):
        total = dot(heads[:, :own_rows], ow[u, 2 * b]) + dot(heads[:, own_rows:], ow[u, 2 * b + 1])
        xh[:, b * lane : (b + 1) * lane] = total.astype(BF16)

    def spread(o):
        return send(xh, xhr.at[o - 1], xh_s.at[o - 1], xh_r.at[o - 1], x_other[o])

    for o in (2, 1, 3):
        spread(o).start()
    add_first(half - 1)
    add_second(half - 2)
    add_second(half - 1)
    for o in (1, 3, 2):
        spread(o).wait_recv()
    near = 2 - 2 * lax.rem(x, 2)
    first = xh[...].astype(F32) + xhr[near].astype(F32)
    attn = first + (xhr[1].astype(F32) + xhr[2 - near].astype(F32))
    left = pl.ds(pl.multiple_of(u * unit, unit), unit)
    hst[u] = (res[:, left].astype(F32) + attn).astype(BF16)
    width = rows.shape[3]
    per_sub = width // unit
    d_model = width * SUBS
    square = jnp.zeros((block, 1), F32)
    for i in range(nz):
        state = hst[i].astype(F32)
        square = square + jnp.sum(state * state, axis=-1, keepdims=True)
    scale = lax.rsqrt(square / d_model + EPS)
    first_expert = 2 * x
    ids = ids_ref[...]
    within = ids - first_expert
    in_group = (within >= 0) & (within < 2)
    is_first = jnp.where(ids == first_expert, 1.0, 0.0)
    lead = jnp.sum(jnp.sum(is_first, axis=1, keepdims=True), axis=0, keepdims=True)
    target = jnp.where(in_group, slots_ref[...] + within * lead.astype(jnp.int32) + GCAP * c, -1)
    row_ids = lax.broadcasted_iota(jnp.int32, (2 * GCAP, block), 0)
    picks = [row_ids == target[k : k + 1, :] for k in range(2)]
    one_hot = jnp.where(picks[0] | picks[1], 1.0, 0.0).astype(BF16)
    share = weights_ref[...].astype(F32) / 65536.0
    mixed = jnp.where(picks[0], share[0:1, :], 0.0) + jnp.where(picks[1], share[1:2, :], 0.0)
    high = mixed.astype(BF16)
    low = (mixed - high.astype(F32)).astype(BF16)
    same = (
        lax.broadcasted_iota(jnp.int32, (block, block), 0)
        == lax.broadcasted_iota(jnp.int32, (block, block), 1)
    )
    turn = jnp.where(same, 1.0, 0.0).astype(BF16)
    for i, piece in enumerate((high, low)):
        mix[i] = lax.dot_general(
            turn, piece, (((1,), (1,)), ((), ())), preferred_element_type=F32
        ).astype(BF16)
    cnt[z, c] = jnp.broadcast_to(lead, cnt.shape[2:])
    to_sibling = send(cnt.at[z, c], cnt.at[z, c], c0_s.at[0], c0_r.at[0], sibling)
    to_sibling.start()
    for k in range(SUBS):
        j = sub_at(k)
        for i in range(per_sub):
            u = j * per_sub + i
            gain = gain_ref[:, pl.ds(pl.multiple_of(u * unit, unit), unit)]
            normed = (hst[u].astype(F32) * scale * gain).astype(BF16)
            own[j, :, i * unit : (i + 1) * unit] = dot(one_hot, normed).astype(BF16)
        send(own.at[j], oth.at[j], ot_s.at[j], ot_r.at[j], sibling).start()
    send(cnt.at[z, 1 - c], cnt.at[z, 1 - c], c0_s.at[0], c0_r.at[0], sibling).wait_recv()
    count_ring(1, z).start()
    for k in range(SUBS):
        j = sub_at(k)
        send(own.at[j], oth.at[j], ot_s.at[j], ot_r.at[j], sibling).wait_recv()
        rows[z, j] = own[j] + oth[j]
        ring2(1, j, z).start()

    for load in loads[5:]:
        load.wait()
    unit_rows = 2 * GCAP
    ffw = wg.shape[1]
    quarter = width // SUBS

    def arrive_count(s, last):
        u = unit_at(-s)
        count_ring(s, u).wait_recv()
        if not last:
            count_ring(s + 1, u).start()
            count_pair(s, u).start()

    def gate_up(k, units):
        j = sub_at(k)
        slab = pl.ds(pl.multiple_of(j * width, width), width)
        block_rows = jnp.concatenate([rows[u, j] for u in units], axis=0)
        many = len(units) * unit_rows
        for i in range(4):
            weight = (wg, wu)[i // 2]
            total = lax.dot_general(
                block_rows, weight[i % 2, :, slab], (((1,), (1,)), ((), ())),
                preferred_element_type=F32,
            )
            if k == 0:
                acc[i, :many] = total
            else:
                acc[i, :many] += total

    def activate(slot, units):
        many = len(units) * unit_rows
        row = lax.broadcasted_iota(jnp.int32, (many, ffw), 0).astype(F32)
        limit = cnt[units[0], 0, 0:1, 0:1]
        start = jnp.zeros((1, 1), F32)
        place = row
        for i in range(1, 2 * len(units)):
            later = row >= i * GCAP
            limit = jnp.where(later, cnt[units[i // 2], i % 2, 0:1, 0:1], limit)
            place = jnp.where(later, row - i * GCAP, place)
        second = place >= limit
        for e in range(2):
            g, up = acc[e, :many], acc[2 + e, :many]
            value = g / (1.0 + jnp.exp(-g)) * up
            mine = second if e == 1 else jnp.logical_not(second)
            hid[slot, e, :many] = jnp.where(mine, value, 0.0).astype(BF16)

    def down(slot, k, units):
        j = sub_at(k)
        many = len(units) * unit_rows
        for f in range(SUBS):
            start = f * width + j * quarter
            cols = pl.ds(pl.multiple_of(start, quarter), quarter)
            total = dot(hid[slot, 0, :many], wd[0, :, cols]) + dot(hid[slot, 1, :many], wd[1, :, cols])
            for i, u in enumerate(units):
                part[u, j, :, f * quarter : (f + 1) * quarter] = total[
                    i * unit_rows : (i + 1) * unit_rows
                ].astype(BF16)

    def both(s):
        return (unit_at(-s), unit_at(s))

    def expert_step(s, carry):
        arrive_count(s, False)
        u = unit_at(-s)
        for k in range(SUBS):
            j = sub_at(k)
            ring2(s, j, u).wait_recv()
            if k < 2:
                ring2(s + 1, j, u).start()
            else:
                @pl.when(s < half - 1)
                def _():
                    ring2(s + 1, j, u).start()
            pair2(s, j, u).start()

            @pl.when(s >= 2)
            def _():
                pair2(s - 1, j, unit_at(s - 1)).wait_recv()

            gate_up(k, both(s - 1))
            if k == SUBS - 1:
                @pl.when(s >= 2)
                def _():
                    count_pair(s - 1, unit_at(s - 1)).wait_recv()

                activate(lax.rem(s - 1, 3), both(s - 1))

            @pl.when(s >= 2)
            def _():
                down(lax.rem(s - 2, 3), k, both(s - 2))

            @pl.when(s >= 3)
            def _():
                give(s - 2, j, unit_at(2 - s)).start()

        return carry

    lax.fori_loop(1, half, expert_step, 0)

    far = unit_at(half)
    arrive_count(half, True)
    for k in range(SUBS):
        pair2(half - 1, sub_at(k), unit_at(half - 1)).wait_recv()
        if k == SUBS - 1:
            ring2(half, sub_at(0), far).wait_recv()
            pair2(half, sub_at(0), far).start()
        gate_up(k, both(half - 1))
    count_pair(half - 1, unit_at(half - 1)).wait_recv()
    activate((half - 1) % 3, both(half - 1))
    for k in range(SUBS):
        down((half - 1) % 3, k, both(half - 1))
        give(half - 1, sub_at(k), unit_at(1 - half)).start()
    ring2(half, sub_at(1), far).wait_recv()
    pair2(half, sub_at(1), far).start()

    def sum_sub(t, k, arrived):
        j = sub_at(k)
        u = unit_at(half - t)
        give(half - t, j, u).wait_recv()
        total = part[u, j].astype(F32) + dbuf[half - t - 1, j].astype(F32)
        if arrived:
            ring3(t, j, u).wait_recv()
            total = total + rbuf[t - 1, j].astype(F32)
        part[u, j] = total.astype(BF16)
        ring3(t + 1, j, u).start()

    sum_sub(1, 2, False)
    sum_sub(1, 3, False)
    single = (far,)
    for k in range(SUBS):
        if k >= 2:
            pair2(half, sub_at(k), far).wait_recv()
        gate_up(k, single)
    activate(half % 3, single)
    for k in (2, 3, 0, 1):
        down(half % 3, k, single)
        if k >= 2:
            give(half, sub_at(k), far).start()
    sum_sub(0, 0, False)
    sum_sub(0, 1, False)
    for k in range(SUBS):
        down((half - 2) % 3, k, both(half - 2))
        if half > 2:
            give(half - 2, sub_at(k), unit_at(2 - half)).start()

    def sum_step(t, carry):
        sum_sub(t + 1, 2, True)
        sum_sub(t + 1, 3, True)
        sum_sub(t, 0, True)
        sum_sub(t, 1, True)
        return carry

    lax.fori_loop(1, half - 1, sum_step, 0)
    sum_sub(half - 1, 0, True)
    sum_sub(half - 1, 1, True)

    def finish(j):
        return send(fin.at[j], finr.at[j], fi_s.at[j], fi_r.at[j], sibling)

    def close(k):
        j = sub_at(k)
        ring3(half, j, z).wait_recv()
        fin[j] = (part[z, j].astype(F32) + rbuf[half - 1, j].astype(F32)).astype(BF16)
        finish(j).start()

    def deliver(j, o):
        at = SUBS * (o - 1) + j
        return send(con.at[at], conr.at[at], co_s.at[at], co_r.at[at], x_other[o])

    def combine(j):
        finish(j).wait_recv()
        for o in (2, 1, 3, 0):
            f = lax.rem(x + o, 4)
            cols = pl.ds(pl.multiple_of(f * quarter, quarter), quarter)
            total = (fin[j, :, cols].astype(F32) + finr[j, :, cols].astype(F32)).astype(BF16)
            moe = dot(mix[0], total) + dot(mix[1], total)
            if o:
                con[SUBS * (o - 1) + j] = moe.astype(BF16)
                deliver(j, o).start()
            else:
                at = j * quarter
                state = hst[x * per_sub + at // unit][:, at % unit : at % unit + quarter]
                own_out[:, at : at + quarter] = state.astype(F32) + moe

    close(2)
    close(3)
    close(0)
    combine(0)
    combine(2)
    close(1)
    combine(1)
    combine(3)
    for j in (0, 2, 1, 3):
        total = own_out[:, j * quarter : (j + 1) * quarter]
        for o in (1, 3, 2):
            deliver(j, o).wait_recv()
            total = total + conr[SUBS * (o - 1) + j].astype(F32)
        out_ref[:, j * quarter : (j + 1) * quarter] = total.astype(BF16)
    for i in range(2):
        send(ow.at[z, i], ow.at[z, i], d0_s.at[i], d0_r.at[i], sibling).wait_send()
    to_sibling.wait_send()

    def drain(s, carry):
        count_ring(s, z).wait_send()
        swap_a(s - 1).wait_send()
        swap_b(s - 1).wait_send()
        for j in range(SUBS):
            @pl.when(s < half)
            def _():
                for make in (ring1, ring2, pair1, pair2, give):
                    make(s, j, z).wait_send()
                ring3(s + 1, j, z).wait_send()

        @pl.when(s < half)
        def _():
            count_pair(s, z).wait_send()

        return carry

    lax.fori_loop(1, half + 1, drain, 0)
    for k in range(2):
        j = sub_at(k)
        for make in (ring1, ring2, pair1, pair2):
            make(half, j, z).wait_send()
        give(half, sub_at(k + 2), z).wait_send()
        ring3(1, j, z).wait_send()
    for j in range(SUBS):
        send(own.at[j], oth.at[j], ot_s.at[j], ot_r.at[j], sibling).wait_send()
        finish(j).wait_send()
    for o in (1, 2, 3):
        spread(o).wait_send()
        for j in range(SUBS):
            deliver(j, o).wait_send()


def per_device(nz, *args):
    (queries, keys, values, out_weight, residual, gain, ids, slots, weights, w_gate, w_up, w_down) = args
    block, heads_width = queries.shape
    d_model = residual.shape[1]
    width = d_model // SUBS
    half = nz // 2
    lane = out_weight.shape[1]
    ow_rows = out_weight.shape[0] // 2
    unit_rows = 2 * GCAP
    ffw = w_gate.shape[2]
    quarter = width // SUBS
    w_gate, w_up = (jnp.swapaxes(w, 1, 2) for w in (w_gate, w_up))
    vmem = pl.BlockSpec(memory_space=pltpu.VMEM)
    hbm = pl.BlockSpec(memory_space=pl.ANY)
    dma = pltpu.SemaphoreType.DMA
    swap = pltpu.VMEM((half, block, 4 * lane), BF16)
    sub = pltpu.VMEM((SUBS, unit_rows, width), BF16)
    scratch = [
        pltpu.VMEM(keys.shape[1:], BF16),
        pltpu.VMEM(values.shape[1:], BF16),
        pltpu.VMEM(residual.shape, BF16),
        pltpu.VMEM(w_gate.shape, BF16),
        pltpu.VMEM(w_up.shape, BF16),
        pltpu.VMEM(w_down.shape, BF16),
        pltpu.VMEM((block, heads_width), BF16),
        pltpu.VMEM((nz, SUBS, ow_rows, lane), BF16),
        swap,
        swap,
        swap,
        swap,
        pltpu.VMEM((nz, block, 2 * lane), BF16),
        sub,
        sub,
        pltpu.VMEM((nz, SUBS, unit_rows, width), BF16),
        pltpu.VMEM((nz, 2, 8, 128), F32),
        pltpu.VMEM((4, 2 * unit_rows, ffw), F32),
        pltpu.VMEM((3, 2, 2 * unit_rows, ffw), BF16),
        pltpu.VMEM((nz, SUBS, unit_rows, width), BF16),
        pltpu.VMEM((half, SUBS, unit_rows, width), BF16),
        pltpu.VMEM((half, SUBS, unit_rows, width), BF16),
        sub,
        sub,
        pltpu.VMEM((3 * SUBS, block, quarter), BF16),
        pltpu.VMEM((3 * SUBS, block, quarter), BF16),
        pltpu.VMEM((block, width), F32),
        pltpu.VMEM((block, 2 * lane), BF16),
        pltpu.VMEM((3, block, 2 * lane), BF16),
        pltpu.VMEM((2, block, unit_rows), BF16),
        dma((8,)),
        dma((2,)),
        dma((2,)),
        *[dma((half + 1, SUBS))] * 4,
        *[dma((half,))] * 4,
        *[dma((SUBS,))] * 2,
        *[dma((half + 1, SUBS))] * 4,
        *[dma((1,))] * 2,
        *[dma((half + 1,))] * 4,
        *[dma((half, SUBS))] * 4,
        *[dma((SUBS,))] * 2,
        *[dma((3 * SUBS,))] * 2,
        *[dma((3,))] * 2,
    ]
    return pl.pallas_call(
        functools.partial(layer_kernel, nz),
        out_shape=jax.ShapeDtypeStruct((block, width), BF16),
        in_specs=[vmem, hbm, hbm, hbm, hbm, vmem, vmem, vmem, vmem, hbm, hbm, hbm],
        out_specs=vmem,
        scratch_shapes=scratch,
        compiler_params=pltpu.CompilerParams(
            collective_id=0, has_side_effects=True, vmem_limit_bytes=67043328
        ),
    )(queries, keys, values, out_weight, residual, gain.reshape(1, -1), ids.T, slots.T, weights.T, w_gate, w_up, w_down)


def solution(mesh):
    in_specs = (
        P(("groups", "fsdp"), "expert"),
        P(("groups", "fsdp"), None, "expert"),
        P(("groups", "fsdp"), None, "expert"),
        P("expert", "fsdp"),
        P(("groups", "fsdp"), None),
        P(),
        P(("groups", "fsdp"), None),
        P(("groups", "fsdp"), None),
        P(("groups", "fsdp"), None),
        P("expert", None, "fsdp"),
        P("expert", None, "fsdp"),
        P("expert", "fsdp", None),
    )
    return jax.shard_map(
        functools.partial(per_device, mesh.shape["fsdp"] // 2),
        mesh=mesh,
        in_specs=in_specs,
        out_specs=P(("groups", "fsdp"), "expert"),
        check_vma=False,
    )
```

```python
import functools

import jax
import jax.numpy as jnp
from jax import lax
from jax.experimental import pallas as pl
from jax.experimental.pallas import tpu as pltpu
from jax.sharding import PartitionSpec as P

HEAD_DIM = 128
GCAP = 36
SUBS = 4
EPS = 1e-05
MESH = pl.DeviceIdType.MESH
F32 = jnp.float32
BF16 = jnp.bfloat16


def dot(a, b):
    return jnp.dot(a, b, preferred_element_type=F32)


def layer_kernel(
    nz,
    q_ref,
    k_hbm,
    v_hbm,
    ow_hbm,
    res_hbm,
    gain_ref,
    ids_ref,
    slots_ref,
    weights_ref,
    wg_hbm,
    wu_hbm,
    wd_hbm,
    out_ref,
    keys,
    vals,
    res,
    wg,
    wu,
    wd,
    heads,
    ow,
    xa,
    xar,
    xb,
    xbr,
    hst,
    own,
    oth,
    rows,
    cnt,
    acc,
    hid,
    part,
    dbuf,
    xin,
    pos,
    posr,
    zsr,
    base,
    finp,
    finpr,
    finz,
    finzr,
    con,
    conr,
    xh,
    xhr,
    mix,
    lsem,
    d0_s,
    d0_r,
    r1_s,
    r1_r,
    d1_s,
    d1_r,
    xa_s,
    xa_r,
    xb_s,
    xb_r,
    ot_s,
    ot_r,
    r2_s,
    r2_r,
    d2_s,
    d2_r,
    c0_s,
    c0_r,
    cr_s,
    cr_r,
    cd_s,
    cd_r,
    db_s,
    db_r,
    xi_s,
    xi_r,
    rs_s,
    rs_r,
    fi_s,
    fi_r,
    co_s,
    co_r,
    xh_s,
    xh_r,
):
    half = nz // 2
    half_width = zsr.shape[3]
    n2 = lax.axis_index("fsdp")
    c = lax.rem(n2, 2)
    z = n2 // 2
    x = lax.axis_index("expert")
    step_dir = 2 * c - 1
    ring_next = {"fsdp": lax.rem(z + step_dir + nz, nz) * 2 + c}
    ring_prev = {"fsdp": lax.rem(z - step_dir + nz, nz) * 2 + c}
    sibling = {"fsdp": z * 2 + 1 - c}
    x_first = {"expert": x + 1 - 2 * lax.rem(x, 2)}
    x_second = {"expert": 3 - x}
    x_other = [{"expert": lax.rem(x + o, 4)} for o in range(4)]

    def unit_at(s):
        return lax.rem(z + s * step_dir + 2 * nz, nz)

    def sub_at(k):
        return lax.rem(2 * c + k, SUBS)

    def send(src, dst, s_sem, r_sem, device):
        return pltpu.make_async_remote_copy(
            src_ref=src, dst_ref=dst, send_sem=s_sem, recv_sem=r_sem,
            device_id=device, device_id_type=MESH,
        )

    def ring1(s, j, u):
        ref = ow.at[u, j]
        return send(ref, ref, r1_s.at[s, j], r1_r.at[s, j], ring_next)

    def pair1(s, j, u):
        ref = ow.at[u, j]
        return send(ref, ref, d1_s.at[s, j], d1_r.at[s, j], sibling)

    def ring2(s, j, u):
        ref = rows.at[u, j]
        return send(ref, ref, r2_s.at[s, j], r2_r.at[s, j], ring_next)

    def pair2(s, j, u):
        ref = rows.at[u, j]
        return send(ref, ref, d2_s.at[s, j], d2_r.at[s, j], sibling)

    def count_ring(s, u):
        return send(cnt.at[u], cnt.at[u], cr_s.at[s], cr_r.at[s], ring_next)

    def count_pair(s, u):
        return send(cnt.at[u], cnt.at[u], cd_s.at[s], cd_r.at[s], sibling)

    def swap_a(s):
        return send(xa.at[s], xar.at[s], xa_s.at[s], xa_r.at[s], x_first)

    def swap_b(s):
        return send(xb.at[s], xbr.at[s], xb_s.at[s], xb_r.at[s], x_second)

    def give(s, j, u):
        return send(part.at[u, j], dbuf.at[s - 1, j], db_s.at[s - 1, j], db_r.at[s - 1, j], sibling)

    def quarter_at(o):
        return lax.rem(x + o, 4)

    def lanes(h):
        return pl.ds(pl.multiple_of(h * half_width, half_width), half_width)

    def ring_p(t, b):
        sems = rs_s.at[t, b], rs_r.at[t, b]
        return send(pos.at[half - t - 1, b], posr.at[t, b], *sems, ring_next)

    def ring_z(t, h):
        sems = rs_s.at[t, 2 + h], rs_r.at[t, 2 + h]
        src = dbuf.at[half - t - 1, quarter_at(2), :, lanes(h)]
        return send(src, zsr.at[t, h], *sems, ring_next)

    def over_far(o):
        i = 1 if o == 1 else 0
        part_rows = pl.ds(pl.multiple_of(32 * c, 32), 40)
        src = dbuf.at[half - 1, quarter_at(o), part_rows]
        dst = xin.at[half, i, part_rows]
        return send(src, dst, xi_s.at[half, i], xi_r.at[half, i], x_other[o])

    def over(s, o, src):
        i = 1 if o == 1 else 0
        return send(src, xin.at[s, i], xi_s.at[s, i], xi_r.at[s, i], x_other[o])

    own_rows = ow_hbm.shape[0] // 2
    loads = [
        pltpu.make_async_copy(ow_hbm.at[pl.ds(0, own_rows)], ow.at[z, 2 * c], lsem.at[0]),
        pltpu.make_async_copy(ow_hbm.at[pl.ds(own_rows, own_rows)], ow.at[z, 2 * c + 1], lsem.at[1]),
        pltpu.make_async_copy(k_hbm.at[0], keys, lsem.at[2]),
        pltpu.make_async_copy(v_hbm.at[0], vals, lsem.at[3]),
        pltpu.make_async_copy(res_hbm, res, lsem.at[4]),
        pltpu.make_async_copy(wg_hbm, wg, lsem.at[5]),
        pltpu.make_async_copy(wu_hbm, wu, lsem.at[6]),
        pltpu.make_async_copy(wd_hbm, wd, lsem.at[7]),
    ]
    for load in loads:
        load.start()

    xin[half] = jnp.zeros(xin.shape[1:], BF16)
    barrier = pltpu.get_barrier_semaphore()
    partners = [ring_next, ring_prev, sibling, *x_other[1:]]
    for device in partners:
        pl.semaphore_signal(barrier, inc=1, device_id=device, device_id_type=MESH)
    pl.semaphore_wait(barrier, len(partners))

    loads[0].wait()
    loads[1].wait()
    for i in range(2):
        j = 2 * c + i
        send(ow.at[z, j], ow.at[z, j], d0_s.at[i], d0_r.at[i], sibling).start()
        ring1(1, j, z).start()
    for i in range(2):
        j = 2 * (1 - c) + i
        send(ow.at[z, j], ow.at[z, j], d0_s.at[i], d0_r.at[i], sibling).wait_recv()
        ring1(1, j, z).start()

    loads[2].wait()
    loads[3].wait()
    block, heads_width = q_ref.shape
    context = keys.shape[0]
    key_pos = lax.broadcasted_iota(jnp.int32, (block, context), 1)
    query_pos = context - block + lax.broadcasted_iota(jnp.int32, (block, context), 0)
    allowed = key_pos <= query_pos
    for h in range(heads_width // HEAD_DIM):
        cols = slice(h * HEAD_DIM, (h + 1) * HEAD_DIM)
        scores = lax.dot_general(
            q_ref[:, cols], keys[...], (((1,), (1,)), ((), ())), preferred_element_type=F32
        ) * HEAD_DIM ** (-0.5)
        masked = jnp.where(allowed, scores, -1e30)
        highest = jnp.max(masked, axis=-1, keepdims=True)
        weights = jnp.where(allowed, jnp.exp(masked - highest), 0.0)
        probs = (weights / jnp.sum(weights, axis=-1, keepdims=True)).astype(BF16)
        heads[:, cols] = dot(probs, vals[...]).astype(BF16)

    unit = 2 * ow.shape[3]
    lane = ow.shape[3]

    def project(s):
        for side, u in enumerate((unit_at(-s), unit_at(s))):
            for b in range(2):
                total = dot(heads[:, :own_rows], ow[u, 2 * b]) + dot(
                    heads[:, own_rows:], ow[u, 2 * b + 1]
                )
                at = side * unit + b * lane
                xa[s, :, at : at + lane] = total.astype(BF16)
        swap_a(s).start()

    def add_first(s):
        swap_a(s).wait_recv()
        xb[s] = (xa[s].astype(F32) + xar[s].astype(F32)).astype(BF16)
        swap_b(s).start()

    def add_second(s):
        swap_b(s).wait_recv()
        for side, u in enumerate((unit_at(-s), unit_at(s))):
            cols = slice(side * unit, (side + 1) * unit)
            attn = xb[s, :, cols].astype(F32) + xbr[s, :, cols].astype(F32)
            left = pl.ds(pl.multiple_of(u * unit, unit), unit)
            hst[u] = (res[:, left].astype(F32) + attn).astype(BF16)

    first_expert = 2 * x
    ids = ids_ref[...]
    within = ids - first_expert
    in_group = (within >= 0) & (within < 2)
    is_first = jnp.where(ids == first_expert, 1.0, 0.0)
    lead = jnp.sum(jnp.sum(is_first, axis=1, keepdims=True), axis=0, keepdims=True)
    target = jnp.where(in_group, slots_ref[...] + within * lead.astype(jnp.int32) + GCAP * c, -1)
    row_ids = lax.broadcasted_iota(jnp.int32, (2 * GCAP, block), 0)
    picks = [row_ids == target[k : k + 1, :] for k in range(2)]
    picked = picks[0] | picks[1]
    one_hot = jnp.where(picked, 1.0, 0.0).astype(BF16)
    share = weights_ref[...].astype(F32) / 65536.0
    share_high = share.astype(BF16).astype(F32)
    facts = [share_high[0:1], share_high[1:2], share[0:1] - share_high[0:1], share[1:2] - share_high[1:2]]
    for o in (3, 1, 0):
        other = 2 * lax.rem(x + o, 4)
        inside = (ids >= other) & (ids < other + 2)
        count = jnp.where(ids == other, 1.0, 0.0)
        count = jnp.sum(jnp.sum(count, axis=1, keepdims=True), axis=0, keepdims=True)
        place = slots_ref[...] + (ids - other) * count.astype(jnp.int32) + GCAP * c + 1
        place = jnp.where(inside, place, 0).astype(F32)
        facts = [place[0:1], place[1:2]] + facts
    shift = (block, cnt.shape[3])
    spot = lax.broadcasted_iota(jnp.int32, shift, 0) + block * c
    placed = spot == lax.broadcasted_iota(jnp.int32, shift, 1)
    same = (
        lax.broadcasted_iota(jnp.int32, (block, block), 0)
        == lax.broadcasted_iota(jnp.int32, (block, block), 1)
    )
    line = lax.broadcasted_iota(jnp.int32, cnt.shape[2:], 0)
    info = jnp.zeros(cnt.shape[2:], F32)
    for i, fact in enumerate(facts):
        column = jnp.sum(jnp.where(same, fact, 0.0), axis=1, keepdims=True)
        wide_fact = jnp.sum(jnp.where(placed, column, 0.0), axis=0, keepdims=True)
        info = jnp.where(line == i + 2, wide_fact, info)
    mixed = jnp.where(picks[0], share[0:1, :], 0.0) + jnp.where(picks[1], share[1:2, :], 0.0)
    high = mixed.astype(BF16)
    low = (mixed - high.astype(F32)).astype(BF16)
    turn = jnp.where(same, 1.0, 0.0).astype(BF16)
    for i, piece in enumerate((high, low)):
        mix[i] = lax.dot_general(
            turn, piece, (((1,), (1,)), ((), ())), preferred_element_type=F32
        ).astype(BF16)
    loads[4].wait()

    def take_pair(s):
        for j in range(SUBS):
            pair1(s, j, unit_at(s)).wait_recv()

    def projection_step(s, carry):
        u = unit_at(-s)
        for k in range(SUBS):
            j = sub_at(k)
            ring1(s, j, u).wait_recv()
            if k < 2:
                ring1(s + 1, j, u).start()
            else:
                @pl.when(s < half - 1)
                def _():
                    ring1(s + 1, j, u).start()
            pair1(s, j, u).start()
            if k == 1:
                @pl.when(s >= 2)
                def _():
                    take_pair(s - 1)

                project(s - 1)

                @pl.when(s >= 2)
                def _():
                    add_first(s - 2)

                @pl.when(s >= 3)
                def _():
                    add_second(s - 3)

        return carry

    lax.fori_loop(1, half, projection_step, 0)
    u = unit_at(half)
    ring1(half, sub_at(0), u).wait_recv()
    pair1(half, sub_at(0), u).start()
    take_pair(half - 1)
    project(half - 1)
    ring1(half, sub_at(1), u).wait_recv()
    pair1(half, sub_at(1), u).start()
    add_first(half - 2)
    if half >= 3:
        add_second(half - 3)
    width = rows.shape[3]
    per_sub = width // unit
    d_model = width * SUBS

    def rows_at(u, k):
        return lax.rem(lax.rem(u + half + 1, nz) // per_sub + 1 + k, SUBS)

    def trade(j):
        return send(own.at[j], oth.at[j], ot_s.at[j], ot_r.at[j], sibling)

    def dispatch(k):
        j = rows_at(z, k)
        for i in range(per_sub):
            u = j * per_sub + i
            gain = gain_ref[:, pl.ds(pl.multiple_of(u * unit, unit), unit)]
            scaled = (hst[u].astype(F32) * gain).astype(BF16)
            own[j, :, i * unit : (i + 1) * unit] = dot(one_hot, scaled).astype(BF16)
        trade(j).start()

    def launch(k):
        j = rows_at(z, k)
        trade(j).wait_recv()
        rows[z, j] = own[j] + oth[j]
        ring2(1, j, z).start()

    add_second(half - 2)
    far = unit_at(half)
    for k in range(2, 4):
        pair1(half, sub_at(k), far).wait_recv()
    for b in range(2):
        total = dot(heads[:, :own_rows], ow[far, 2 * b]) + dot(
            heads[:, own_rows:], ow[far, 2 * b + 1]
        )
        xh[:, b * lane : (b + 1) * lane] = total.astype(BF16)

    def spread(o):
        return send(xh, xhr.at[o - 1], xh_s.at[o - 1], xh_r.at[o - 1], x_other[o])

    for o in (2, 1, 3):
        spread(o).start()
    dispatch(0)
    dispatch(1)
    add_first(half - 1)
    launch(0)
    launch(1)
    add_second(half - 1)
    for o in (1, 3, 2):
        spread(o).wait_recv()
    near = 2 - 2 * lax.rem(x, 2)
    first = xh[...].astype(F32) + xhr[near].astype(F32)
    attn = first + (xhr[1].astype(F32) + xhr[2 - near].astype(F32))
    left = pl.ds(pl.multiple_of(far * unit, unit), unit)
    hst[far] = (res[:, left].astype(F32) + attn).astype(BF16)
    dispatch(2)
    dispatch(3)
    square = jnp.zeros((block, 1), F32)
    for i in range(nz):
        state = hst[i].astype(F32)
        square = square + jnp.sum(state * state, axis=-1, keepdims=True)
    scale = lax.rsqrt(square / d_model + EPS)
    by_position = jnp.sum(jnp.where(same, scale, 0.0), axis=0, keepdims=True)
    by_row = jnp.sum(jnp.where(picked, by_position, 0.0), axis=1, keepdims=True)
    grid = (2 * GCAP, cnt.shape[3])
    diagonal = lax.broadcasted_iota(jnp.int32, grid, 0) == lax.broadcasted_iota(jnp.int32, grid, 1)
    row_scale = jnp.sum(jnp.where(diagonal, by_row, 0.0), axis=0, keepdims=True)
    cnt[z, c] = jnp.where(line == 0, lead, jnp.where(line == 1, row_scale, info))
    to_sibling = send(cnt.at[z, c], cnt.at[z, c], c0_s.at[0], c0_r.at[0], sibling)
    to_sibling.start()
    launch(2)
    launch(3)
    send(cnt.at[z, 1 - c], cnt.at[z, 1 - c], c0_s.at[0], c0_r.at[0], sibling).wait_recv()
    count_ring(1, z).start()
    for load in loads[5:]:
        load.wait()
    unit_rows = 2 * GCAP
    ffw = wg.shape[1]
    quarter = width // SUBS

    def arrive_count(s, last):
        u = unit_at(-s)
        count_ring(s, u).wait_recv()
        if not last:
            count_ring(s + 1, u).start()
            count_pair(s, u).start()

    def gate_up(j, units, first):
        slab = pl.ds(j * width, width) if isinstance(j, int) else pl.ds(
            pl.multiple_of(j * width, width), width
        )
        block_rows = jnp.concatenate([rows[u, j] for u in units], axis=0)
        many = len(units) * unit_rows
        for i in range(4):
            weight = (wg, wu)[i // 2]
            total = lax.dot_general(
                block_rows, weight[i % 2, :, slab], (((1,), (1,)), ((), ())),
                preferred_element_type=F32,
            )
            if first:
                acc[i, :many] = total
            else:
                acc[i, :many] += total

    def activate(slot, units):
        many = len(units) * unit_rows
        row = lax.broadcasted_iota(jnp.int32, (many, ffw), 0).astype(F32)
        limit = cnt[units[0], 0, 0:1, 0:1]
        place = row
        for i in range(1, 2 * len(units)):
            later = row >= i * GCAP
            limit = jnp.where(later, cnt[units[i // 2], i % 2, 0:1, 0:1], limit)
            place = jnp.where(later, row - i * GCAP, place)
        second = place >= limit
        wide = (many, cnt.shape[3])
        at = lax.broadcasted_iota(jnp.int32, wide, 0) - lax.broadcasted_iota(jnp.int32, wide, 1)
        factor = jnp.zeros(wide, F32)
        for i, u in enumerate(units):
            row_scale = cnt[u, 0, 1:2, :] + cnt[u, 1, 1:2, :]
            factor = factor + jnp.where(at == i * unit_rows, row_scale, 0.0)
        factor = jnp.sum(factor, axis=1, keepdims=True)
        for e in range(2):
            g, up = acc[e, :many] * factor, acc[2 + e, :many] * factor
            value = g / (1.0 + jnp.exp(-g)) * up
            mine = second if e == 1 else jnp.logical_not(second)
            hid[slot, e, :many] = jnp.where(mine, value, 0.0).astype(BF16)

    def down(slot, f, units):
        many = len(units) * unit_rows
        for i in range(SUBS):
            start = f * width + i * quarter
            if not isinstance(f, int):
                start = pl.multiple_of(start, quarter)
            cols = pl.ds(start, quarter)
            total = dot(hid[slot, 0, :many], wd[0, :, cols]) + dot(hid[slot, 1, :many], wd[1, :, cols])
            for n, u in enumerate(units):
                part[u, f, :, i * quarter : (i + 1) * quarter] = total[
                    n * unit_rows : (n + 1) * unit_rows
                ].astype(BF16)

    def both(s):
        return (unit_at(-s), unit_at(s))

    def prepare(s, last=False):
        u = unit_at(s)
        for o in (1, 3, 2, 0):
            f = quarter_at(o)
            give(s, f, u).wait_recv()
            dbuf[s - 1, f] = (part[u, f].astype(F32) + dbuf[s - 1, f].astype(F32)).astype(BF16)
            if o in (1, 3):
                (over_far(o) if last else over(s, o, dbuf.at[s - 1, f])).start()

    def by_positions(s, mine, last=False):
        for o in (1, 3):
            (over_far(o) if last else over(s, o, xin.at[s, 0])).wait_recv()
        u = unit_at(s)
        facts = cnt[u, 0] + cnt[u, 1]
        row = lax.broadcasted_iota(jnp.int32, (unit_rows, cnt.shape[3]), 0).astype(F32) + 1.0
        highs, lows = [], []
        for i in range(3):
            hit = [row == facts[2 + 2 * i + k : 3 + 2 * i + k] for k in range(2)]
            for kept, at in ((highs, 8), (lows, 10)):
                kept.append(
                    jnp.where(hit[0], facts[at : at + 1], 0.0)
                    + jnp.where(hit[1], facts[at + 1 : at + 2], 0.0)
                )
        sums = jnp.concatenate([mine, xin[s, 0], xin[s, 1]], axis=0)
        total = None
        for weight in (highs, lows):
            turned = jnp.transpose(jnp.concatenate(weight, axis=0)).astype(BF16)
            term = dot(turned, sums)
            total = term if total is None else total + term
        return total

    def gather_positions(s, last=False):
        total = by_positions(s, dbuf[s - 1, x], last)
        for b in range(2):
            pos[s - 1, b] = total[b * block : (b + 1) * block].astype(BF16)

    def sum_p(t, b, arrived):
        if arrived:
            ring_p(t - 1, b).wait_recv()
            at = half - t - 1
            pos[at, b] = (pos[at, b].astype(F32) + posr[t - 1, b].astype(F32)).astype(BF16)
        ring_p(t, b).start()

    def sum_z(t, h, arrived):
        if arrived:
            ring_z(t - 1, h).wait_recv()
            at = half - t - 1
            f = quarter_at(2)
            dbuf[at, f, :, lanes(h)] = (
                dbuf[at, f, :, lanes(h)].astype(F32) + zsr[t - 1, h].astype(F32)
            ).astype(BF16)
        ring_z(t, h).start()

    def expert_step(s, carry):
        u = unit_at(-s)
        for k in range(SUBS):
            j = rows_at(u, k)
            ring2(s, j, u).wait_recv()

            @pl.when((s < half - 1) | (c == 1 if k < 2 else c == 0))
            def _():
                ring2(s + 1, j, u).start()

            pair2(s, j, u).start()
            if k == 2:
                arrive_count(s, False)
            @pl.when(s >= 2)
            def _():
                pair2(s - 1, k, unit_at(s - 1)).wait_recv()

            gate_up(k, both(s - 1), k == 0)
            if k == SUBS - 1:
                @pl.when(s >= 2)
                def _():
                    count_pair(s - 1, unit_at(s - 1)).wait_recv()

                activate(lax.rem(s - 1, 3), both(s - 1))

            @pl.when(s >= 2)
            def _():
                down(lax.rem(s - 2, 3), k, both(s - 2))

            @pl.when(s >= 3)
            def _():
                give(s - 2, k, unit_at(2 - s)).start()

        @pl.when(s == 3)
        def _():
            for o in (1, 3):
                over(0, o, part.at[z, quarter_at(o)]).start()

        @pl.when(s >= 4)
        def _():
            prepare(s - 3)

        return carry

    lax.fori_loop(1, half, expert_step, 0)

    own_far = [rows_at(far, 2 * (1 - c) + i) for i in range(2)]
    other_far = [rows_at(far, 2 * c + i) for i in range(2)]
    prepare(half - 3)
    for k in range(SUBS):
        pair2(half - 1, k, unit_at(half - 1)).wait_recv()
        if k == SUBS - 1:
            ring2(half, own_far[0], far).wait_recv()
            pair2(half, own_far[0], far).start()
        gate_up(k, both(half - 1), k == 0)
    count_pair(half - 1, unit_at(half - 1)).wait_recv()
    activate((half - 1) % 3, both(half - 1))
    for o in (1, 3, 2, 0):
        down((half - 1) % 3, quarter_at(o), both(half - 1))
        give(half - 1, quarter_at(o), unit_at(1 - half)).start()
    ring2(half, own_far[1], far).wait_recv()
    pair2(half, own_far[1], far).start()
    arrive_count(half, True)

    prepare(half - 1)
    sum_z(1, 1 - c, False)
    single = (far,)
    for i in range(2):
        gate_up(own_far[i], single, i == 0)
    for i in range(2):
        pair2(half, other_far[i], far).wait_recv()
        gate_up(other_far[i], single, False)
    activate(half % 3, single)
    for o in (1, 3, 2, 0):
        down(half % 3, quarter_at(o), single)
        give(half, quarter_at(o), far).start()
    prepare(half, True)
    sum_z(0, c, False)
    gather_positions(half - 1)
    sum_p(1, 1 - c, False)
    for o in (1, 3, 2, 0):
        down((half - 2) % 3, quarter_at(o), both(half - 2))
        give(half - 2, quarter_at(o), unit_at(2 - half)).start()
    prepare(half - 2)
    sum_z(2, 1 - c, True)
    gather_positions(half, True)
    sum_p(0, c, False)
    sum_z(1, c, True)
    total = by_positions(0, part[z, x])
    for b in range(2):
        base[b] = total[b * block : (b + 1) * block]

    def sum_step(t, carry):
        @pl.when(t < half)
        def _():
            sum_z(t, 1 - c, True)

        gather_positions(half - t + 1)
        sum_z(t - 1, c, True)
        sum_p(t - 1, 1 - c, True)
        sum_p(t - 2, c, True)
        return carry

    lax.fori_loop(3, half + 1, sum_step, 0)

    def swap_z(h):
        return send(finz.at[h], finzr.at[h], fi_s.at[h], fi_r.at[h], sibling)

    swap_p = send(finp, finpr, fi_s.at[2], fi_r.at[2], sibling)

    def close_z(h):
        ring_z(half - 1, h).wait_recv()
        own_part = part[z, quarter_at(2), :, lanes(h)]
        finz[h] = (own_part.astype(F32) + zsr[half - 1, h].astype(F32)).astype(BF16)
        swap_z(h).start()

    def deliver(h):
        return send(con.at[h], conr.at[h], co_s.at[h], co_r.at[h], x_other[2])

    def cross(h):
        swap_z(h).wait_recv()
        total = (finz[h].astype(F32) + finzr[h].astype(F32)).astype(BF16)
        con[h] = (dot(mix[0], total) + dot(mix[1], total)).astype(BF16)
        deliver(h).start()

    close_z(1 - c)
    sum_p(half - 1, c, True)
    close_z(c)
    cross(0)
    cross(1)
    ring_p(half - 1, 1 - c).wait_recv()
    finp[...] = (base[1 - c] + posr[half - 1, 1 - c].astype(F32)).astype(BF16)
    swap_p.start()
    ring_p(half - 1, c).wait_recv()
    swap_p.wait_recv()
    base[c] = base[c] + posr[half - 1, c].astype(F32) + finpr[...].astype(F32)
    for h in range(2):
        deliver(h).wait_recv()
        for i in range(half_width // min(unit, half_width)):
            step = min(unit, half_width)
            at = h * half_width + i * step
            state = hst[x * per_sub + at // unit][:, at % unit : at % unit + step]
            total = state.astype(F32) + base[c, :, at : at + step]
            total = total + conr[h, :, i * step : (i + 1) * step].astype(F32)
            out_ref[:, at : at + step] = total.astype(BF16)
    for i in range(2):
        send(ow.at[z, i], ow.at[z, i], d0_s.at[i], d0_r.at[i], sibling).wait_send()
    to_sibling.wait_send()

    def drain(s, carry):
        count_ring(s, z).wait_send()
        swap_a(s - 1).wait_send()
        swap_b(s - 1).wait_send()
        for j in range(SUBS):
            @pl.when(s < half)
            def _():
                for make in (ring1, ring2, pair1, pair2):
                    make(s, j, z).wait_send()

            give(s, j, z).wait_send()

        @pl.when(s < half)
        def _():
            for o in (1, 3):
                over(s, o, xin.at[s, 0]).wait_send()
            count_pair(s, z).wait_send()
            for b in range(2):
                ring_p(s, b).wait_send()
                ring_z(s, b).wait_send()

        return carry

    lax.fori_loop(1, half + 1, drain, 0)
    for k in range(2):
        j = sub_at(k)
        for make in (ring1, pair1):
            make(half, j, z).wait_send()
        ring2(half, rows_at(unit_at(1 - half), 2 * (1 - c) + k), z).wait_send()
        pair2(half, own_far[k], z).wait_send()
        deliver(k).wait_send()
        swap_z(k).wait_send()
        over(0, 1 + 2 * k, xin.at[0, 0]).wait_send()
        over_far(1 + 2 * k).wait_send()
    for j in range(SUBS):
        send(own.at[j], oth.at[j], ot_s.at[j], ot_r.at[j], sibling).wait_send()
    for o in (1, 2, 3):
        spread(o).wait_send()
    ring_p(0, c).wait_send()
    ring_z(0, c).wait_send()
    swap_p.wait_send()


def per_device(nz, *args):
    (queries, keys, values, out_weight, residual, gain, ids, slots, weights, w_gate, w_up, w_down) = args
    block, heads_width = queries.shape
    d_model = residual.shape[1]
    width = d_model // SUBS
    half = nz // 2
    lane = out_weight.shape[1]
    ow_rows = out_weight.shape[0] // 2
    unit_rows = 2 * GCAP
    ffw = w_gate.shape[2]
    w_gate, w_up = (jnp.swapaxes(w, 1, 2) for w in (w_gate, w_up))
    vmem = pl.BlockSpec(memory_space=pltpu.VMEM)
    hbm = pl.BlockSpec(memory_space=pl.ANY)
    dma = pltpu.SemaphoreType.DMA
    swap = pltpu.VMEM((half, block, 4 * lane), BF16)
    sub = pltpu.VMEM((SUBS, unit_rows, width), BF16)
    scratch = [
        pltpu.VMEM(keys.shape[1:], BF16),
        pltpu.VMEM(values.shape[1:], BF16),
        pltpu.VMEM(residual.shape, BF16),
        pltpu.VMEM(w_gate.shape, BF16),
        pltpu.VMEM(w_up.shape, BF16),
        pltpu.VMEM(w_down.shape, BF16),
        pltpu.VMEM((block, heads_width), BF16),
        pltpu.VMEM((nz, SUBS, ow_rows, lane), BF16),
        swap,
        swap,
        swap,
        swap,
        pltpu.VMEM((nz, block, 2 * lane), BF16),
        sub,
        sub,
        pltpu.VMEM((nz, SUBS, unit_rows, width), BF16),
        pltpu.VMEM((nz, 2, 16, 128), F32),
        pltpu.VMEM((4, 2 * unit_rows, ffw), F32),
        pltpu.VMEM((3, 2, 2 * unit_rows, ffw), BF16),
        pltpu.VMEM((nz, SUBS, unit_rows, width), BF16),
        pltpu.VMEM((half, SUBS, unit_rows, width), BF16),
        pltpu.VMEM((half + 1, 2, unit_rows, width), BF16),
        pltpu.VMEM((half, 2, block, width), BF16),
        pltpu.VMEM((half, 2, block, width), BF16),
        pltpu.VMEM((half, 2, unit_rows, width // 2), BF16),
        pltpu.VMEM((2, block, width), F32),
        *[pltpu.VMEM((block, width), BF16)] * 2,
        *[pltpu.VMEM((2, unit_rows, width // 2), BF16)] * 2,
        *[pltpu.VMEM((2, block, width // 2), BF16)] * 2,
        pltpu.VMEM((block, 2 * lane), BF16),
        pltpu.VMEM((3, block, 2 * lane), BF16),
        pltpu.VMEM((2, block, unit_rows), BF16),
        dma((8,)),
        dma((2,)),
        dma((2,)),
        *[dma((half + 1, SUBS))] * 4,
        *[dma((half,))] * 4,
        *[dma((SUBS,))] * 2,
        *[dma((half + 1, SUBS))] * 4,
        *[dma((1,))] * 2,
        *[dma((half + 1,))] * 4,
        *[dma((half, SUBS))] * 2,
        *[dma((half + 1, 2))] * 2,
        *[dma((half, SUBS))] * 2,
        *[dma((3,))] * 2,
        *[dma((2,))] * 2,
        *[dma((3,))] * 2,
    ]
    return pl.pallas_call(
        functools.partial(layer_kernel, nz),
        out_shape=jax.ShapeDtypeStruct((block, width), BF16),
        in_specs=[vmem, hbm, hbm, hbm, hbm, vmem, vmem, vmem, vmem, hbm, hbm, hbm],
        out_specs=vmem,
        scratch_shapes=scratch,
        compiler_params=pltpu.CompilerParams(
            collective_id=0, has_side_effects=True, vmem_limit_bytes=67043328
        ),
    )(queries, keys, values, out_weight, residual, gain.reshape(1, -1), ids.T, slots.T, weights.T, w_gate, w_up, w_down)


def solution(mesh):
    in_specs = (
        P(("groups", "fsdp"), "expert"),
        P(("groups", "fsdp"), None, "expert"),
        P(("groups", "fsdp"), None, "expert"),
        P("expert", "fsdp"),
        P(("groups", "fsdp"), None),
        P(),
        P(("groups", "fsdp"), None),
        P(("groups", "fsdp"), None),
        P(("groups", "fsdp"), None),
        P("expert", None, "fsdp"),
        P("expert", None, "fsdp"),
        P("expert", "fsdp", None),
    )
    return jax.shard_map(
        functools.partial(per_device, mesh.shape["fsdp"] // 2),
        mesh=mesh,
        in_specs=in_specs,
        out_specs=P(("groups", "fsdp"), "expert"),
        check_vma=False,
    )
```

```python
import functools

import jax
import jax.numpy as jnp
from jax import lax
from jax.experimental import pallas as pl
from jax.experimental.pallas import tpu as pltpu
from jax.sharding import PartitionSpec as P

HEAD_DIM = 128
GCAP = 36
SUBS = 4
EPS = 1e-05
MESH = pl.DeviceIdType.MESH
F32 = jnp.float32
BF16 = jnp.bfloat16


def dot(a, b):
    return jnp.dot(a, b, preferred_element_type=F32)


def layer_kernel(
    nz,
    q_ref,
    k_hbm,
    v_hbm,
    ow_hbm,
    res_hbm,
    gain_ref,
    ids_ref,
    slots_ref,
    weights_ref,
    wg_hbm,
    wu_hbm,
    wd_hbm,
    out_ref,
    keys,
    vals,
    res,
    wg,
    wu,
    wd,
    stage,
    heads,
    ow,
    xa,
    xar,
    xb,
    xbr,
    hst,
    own,
    oth,
    rows,
    cnt,
    acc,
    hid,
    part,
    dbuf,
    xin,
    pos,
    posr,
    zsr,
    base,
    finp,
    finpr,
    finz,
    finzr,
    con,
    conr,
    xh,
    xhr,
    mix,
    lsem,
    wsem,
    d0_s,
    d0_r,
    r1_s,
    r1_r,
    d1_s,
    d1_r,
    xa_s,
    xa_r,
    xb_s,
    xb_r,
    ot_s,
    ot_r,
    r2_s,
    r2_r,
    d2_s,
    d2_r,
    c0_s,
    c0_r,
    cr_s,
    cr_r,
    cd_s,
    cd_r,
    db_s,
    db_r,
    xi_s,
    xi_r,
    rs_s,
    rs_r,
    fi_s,
    fi_r,
    co_s,
    co_r,
    xh_s,
    xh_r,
):
    half = nz // 2
    half_width = zsr.shape[3]
    n2 = lax.axis_index("fsdp")
    c = lax.rem(n2, 2)
    z = n2 // 2
    x = lax.axis_index("expert")
    step_dir = 2 * c - 1
    ring_next = {"fsdp": lax.rem(z + step_dir + nz, nz) * 2 + c}
    ring_prev = {"fsdp": lax.rem(z - step_dir + nz, nz) * 2 + c}
    sibling = {"fsdp": z * 2 + 1 - c}
    x_first = {"expert": x + 1 - 2 * lax.rem(x, 2)}
    x_second = {"expert": 3 - x}
    x_other = [{"expert": lax.rem(x + o, 4)} for o in range(4)]

    def unit_at(s):
        return lax.rem(z + s * step_dir + 2 * nz, nz)

    def sub_at(k):
        return lax.rem(2 * c + k, SUBS)

    def send(src, dst, s_sem, r_sem, device):
        return pltpu.make_async_remote_copy(
            src_ref=src, dst_ref=dst, send_sem=s_sem, recv_sem=r_sem,
            device_id=device, device_id_type=MESH,
        )

    def ring1(s, j, u):
        ref = ow.at[u, j]
        return send(ref, ref, r1_s.at[s, j], r1_r.at[s, j], ring_next)

    def pair1(s, j, u):
        ref = ow.at[u, j]
        return send(ref, ref, d1_s.at[s, j], d1_r.at[s, j], sibling)

    def ring2(s, j, u):
        ref = rows.at[u, j]
        return send(ref, ref, r2_s.at[s, j], r2_r.at[s, j], ring_next)

    def pair2(s, j, u):
        ref = rows.at[u, j]
        return send(ref, ref, d2_s.at[s, j], d2_r.at[s, j], sibling)

    def count_ring(s, u):
        return send(cnt.at[u], cnt.at[u], cr_s.at[s], cr_r.at[s], ring_next)

    def count_pair(s, u):
        return send(cnt.at[u], cnt.at[u], cd_s.at[s], cd_r.at[s], sibling)

    def swap_a(s):
        return send(xa.at[s], xar.at[s], xa_s.at[s], xa_r.at[s], x_first)

    def swap_b(s):
        return send(xb.at[s], xbr.at[s], xb_s.at[s], xb_r.at[s], x_second)

    def give(s, j, u):
        return send(part.at[u, j], dbuf.at[s - 1, j], db_s.at[s - 1, j], db_r.at[s - 1, j], sibling)

    def quarter_at(o):
        return lax.rem(x + o, 4)

    def lanes(h):
        return pl.ds(pl.multiple_of(h * half_width, half_width), half_width)

    def ring_p(t, b):
        sems = rs_s.at[t, b], rs_r.at[t, b]
        return send(pos.at[half - t - 1, b], posr.at[t, b], *sems, ring_next)

    def ring_z(t, h):
        sems = rs_s.at[t, 2 + h], rs_r.at[t, 2 + h]
        src = dbuf.at[half - t - 1, quarter_at(2), :, lanes(h)]
        return send(src, zsr.at[t, h], *sems, ring_next)

    def over_far(o):
        i = 1 if o == 1 else 0
        part_rows = pl.ds(pl.multiple_of(32 * c, 32), 40)
        src = dbuf.at[half - 1, quarter_at(o), part_rows]
        dst = xin.at[half, i, part_rows]
        return send(src, dst, xi_s.at[half, i], xi_r.at[half, i], x_other[o])

    def over(s, o, src):
        i = 1 if o == 1 else 0
        return send(src, xin.at[s, i], xi_s.at[s, i], xi_r.at[s, i], x_other[o])

    own_rows = ow_hbm.shape[0] // 2
    loads = [
        pltpu.make_async_copy(ow_hbm.at[pl.ds(0, own_rows)], ow.at[z, 2 * c], lsem.at[0]),
        pltpu.make_async_copy(ow_hbm.at[pl.ds(own_rows, own_rows)], ow.at[z, 2 * c + 1], lsem.at[1]),
        pltpu.make_async_copy(k_hbm.at[0], keys, lsem.at[2]),
        pltpu.make_async_copy(v_hbm.at[0], vals, lsem.at[3]),
        pltpu.make_async_copy(res_hbm, res, lsem.at[4]),
        pltpu.make_async_copy(wd_hbm, wd, lsem.at[5]),
    ]

    slabs = 2 * SUBS
    slab_width = stage.shape[3]

    def slab_load(m, i):
        cols = pl.ds(pl.multiple_of((i % SUBS) * slab_width, slab_width), slab_width)
        src = (wg_hbm, wu_hbm)[m].at[i // SUBS, :, cols]
        return pltpu.make_async_copy(src, stage.at[m, i % 2], wsem.at[m, i % 2])

    def turn_slab(m, i):
        slab_load(m, i).wait()
        at = pl.ds(pl.multiple_of((i % SUBS) * slab_width, slab_width), slab_width)
        (wg, wu)[m][i // SUBS, at, :] = jnp.transpose(stage[m, i % 2])

        @pl.when(i + 2 < slabs)
        def _():
            slab_load(m, i + 2).start()

    for load in loads[:5]:
        load.start()
    for i in range(2):
        for m in range(2):
            slab_load(m, jnp.int32(i)).start()
    loads[5].start()

    xin[half] = jnp.zeros(xin.shape[1:], BF16)
    barrier = pltpu.get_barrier_semaphore()
    partners = [ring_next, ring_prev, sibling, *x_other[1:]]
    for device in partners:
        pl.semaphore_signal(barrier, inc=1, device_id=device, device_id_type=MESH)
    pl.semaphore_wait(barrier, len(partners))

    loads[0].wait()
    loads[1].wait()
    for i in range(2):
        j = 2 * c + i
        send(ow.at[z, j], ow.at[z, j], d0_s.at[i], d0_r.at[i], sibling).start()
        ring1(1, j, z).start()
    for i in range(2):
        j = 2 * (1 - c) + i
        send(ow.at[z, j], ow.at[z, j], d0_s.at[i], d0_r.at[i], sibling).wait_recv()
        ring1(1, j, z).start()

    loads[2].wait()
    loads[3].wait()
    block, heads_width = q_ref.shape
    context = keys.shape[0]
    key_pos = lax.broadcasted_iota(jnp.int32, (block, context), 1)
    query_pos = context - block + lax.broadcasted_iota(jnp.int32, (block, context), 0)
    allowed = key_pos <= query_pos
    for h in range(heads_width // HEAD_DIM):
        cols = slice(h * HEAD_DIM, (h + 1) * HEAD_DIM)
        scores = lax.dot_general(
            q_ref[:, cols], keys[...], (((1,), (1,)), ((), ())), preferred_element_type=F32
        ) * HEAD_DIM ** (-0.5)
        masked = jnp.where(allowed, scores, -1e30)
        highest = jnp.max(masked, axis=-1, keepdims=True)
        weights = jnp.where(allowed, jnp.exp(masked - highest), 0.0)
        probs = (weights / jnp.sum(weights, axis=-1, keepdims=True)).astype(BF16)
        heads[:, cols] = dot(probs, vals[...]).astype(BF16)

    unit = 2 * ow.shape[3]
    lane = ow.shape[3]

    def project(s):
        for side, u in enumerate((unit_at(-s), unit_at(s))):
            for b in range(2):
                total = dot(heads[:, :own_rows], ow[u, 2 * b]) + dot(
                    heads[:, own_rows:], ow[u, 2 * b + 1]
                )
                at = side * unit + b * lane
                xa[s, :, at : at + lane] = total.astype(BF16)
        swap_a(s).start()

    def add_first(s):
        swap_a(s).wait_recv()
        xb[s] = (xa[s].astype(F32) + xar[s].astype(F32)).astype(BF16)
        swap_b(s).start()

    def add_second(s):
        swap_b(s).wait_recv()
        for side, u in enumerate((unit_at(-s), unit_at(s))):
            cols = slice(side * unit, (side + 1) * unit)
            attn = xb[s, :, cols].astype(F32) + xbr[s, :, cols].astype(F32)
            left = pl.ds(pl.multiple_of(u * unit, unit), unit)
            hst[u] = (res[:, left].astype(F32) + attn).astype(BF16)

    first_expert = 2 * x
    ids = ids_ref[...]
    within = ids - first_expert
    in_group = (within >= 0) & (within < 2)
    is_first = jnp.where(ids == first_expert, 1.0, 0.0)
    lead = jnp.sum(jnp.sum(is_first, axis=1, keepdims=True), axis=0, keepdims=True)
    target = jnp.where(in_group, slots_ref[...] + within * lead.astype(jnp.int32) + GCAP * c, -1)
    row_ids = lax.broadcasted_iota(jnp.int32, (2 * GCAP, block), 0)
    picks = [row_ids == target[k : k + 1, :] for k in range(2)]
    picked = picks[0] | picks[1]
    one_hot = jnp.where(picked, 1.0, 0.0).astype(BF16)
    share = weights_ref[...].astype(F32) / 65536.0
    share_high = share.astype(BF16).astype(F32)
    facts = [share_high[0:1], share_high[1:2], share[0:1] - share_high[0:1], share[1:2] - share_high[1:2]]
    for o in (3, 1, 0):
        other = 2 * lax.rem(x + o, 4)
        inside = (ids >= other) & (ids < other + 2)
        count = jnp.where(ids == other, 1.0, 0.0)
        count = jnp.sum(jnp.sum(count, axis=1, keepdims=True), axis=0, keepdims=True)
        place = slots_ref[...] + (ids - other) * count.astype(jnp.int32) + GCAP * c + 1
        place = jnp.where(inside, place, 0).astype(F32)
        facts = [place[0:1], place[1:2]] + facts
    shift = (block, cnt.shape[3])
    spot = lax.broadcasted_iota(jnp.int32, shift, 0) + block * c
    placed = spot == lax.broadcasted_iota(jnp.int32, shift, 1)
    same = (
        lax.broadcasted_iota(jnp.int32, (block, block), 0)
        == lax.broadcasted_iota(jnp.int32, (block, block), 1)
    )
    line = lax.broadcasted_iota(jnp.int32, cnt.shape[2:], 0)
    info = jnp.zeros(cnt.shape[2:], F32)
    for i, fact in enumerate(facts):
        column = jnp.sum(jnp.where(same, fact, 0.0), axis=1, keepdims=True)
        wide_fact = jnp.sum(jnp.where(placed, column, 0.0), axis=0, keepdims=True)
        info = jnp.where(line == i + 2, wide_fact, info)
    mixed = jnp.where(picks[0], share[0:1, :], 0.0) + jnp.where(picks[1], share[1:2, :], 0.0)
    high = mixed.astype(BF16)
    low = (mixed - high.astype(F32)).astype(BF16)
    turn = jnp.where(same, 1.0, 0.0).astype(BF16)
    for i, piece in enumerate((high, low)):
        mix[i] = lax.dot_general(
            turn, piece, (((1,), (1,)), ((), ())), preferred_element_type=F32
        ).astype(BF16)
    loads[4].wait()

    def take_pair(s):
        for j in range(SUBS):
            pair1(s, j, unit_at(s)).wait_recv()

    def projection_step(s, carry):
        u = unit_at(-s)
        for k in range(SUBS):
            j = sub_at(k)
            ring1(s, j, u).wait_recv()
            if k < 2:
                ring1(s + 1, j, u).start()
            else:
                @pl.when(s < half - 1)
                def _():
                    ring1(s + 1, j, u).start()
            pair1(s, j, u).start()
            if k in (0, 2):
                turn_slab(k // 2, s - 1)
            if k == 1:
                @pl.when(s >= 2)
                def _():
                    take_pair(s - 1)

                project(s - 1)

                @pl.when(s >= 2)
                def _():
                    add_first(s - 2)

                @pl.when(s >= 3)
                def _():
                    add_second(s - 3)

        return carry

    lax.fori_loop(1, half, projection_step, 0)
    u = unit_at(half)
    ring1(half, sub_at(0), u).wait_recv()
    pair1(half, sub_at(0), u).start()
    take_pair(half - 1)
    project(half - 1)
    ring1(half, sub_at(1), u).wait_recv()
    pair1(half, sub_at(1), u).start()
    add_first(half - 2)
    if half >= 3:
        add_second(half - 3)
    width = rows.shape[3]
    per_sub = width // unit
    d_model = width * SUBS

    def rows_at(u, k):
        return lax.rem(lax.rem(u + half + 1, nz) // per_sub + 1 + k, SUBS)

    def trade(j):
        return send(own.at[j], oth.at[j], ot_s.at[j], ot_r.at[j], sibling)

    def dispatch(k):
        j = rows_at(z, k)
        for i in range(per_sub):
            u = j * per_sub + i
            gain = gain_ref[:, pl.ds(pl.multiple_of(u * unit, unit), unit)]
            scaled = (hst[u].astype(F32) * gain).astype(BF16)
            own[j, :, i * unit : (i + 1) * unit] = dot(one_hot, scaled).astype(BF16)
        trade(j).start()

    def launch(k):
        j = rows_at(z, k)
        trade(j).wait_recv()
        rows[z, j] = own[j] + oth[j]
        ring2(1, j, z).start()

    add_second(half - 2)
    far = unit_at(half)
    for k in range(2, 4):
        pair1(half, sub_at(k), far).wait_recv()
    for b in range(2):
        total = dot(heads[:, :own_rows], ow[far, 2 * b]) + dot(
            heads[:, own_rows:], ow[far, 2 * b + 1]
        )
        xh[:, b * lane : (b + 1) * lane] = total.astype(BF16)

    def spread(o):
        return send(xh, xhr.at[o - 1], xh_s.at[o - 1], xh_r.at[o - 1], x_other[o])

    for o in (2, 1, 3):
        spread(o).start()
    dispatch(0)
    dispatch(1)
    add_first(half - 1)
    launch(0)
    launch(1)
    add_second(half - 1)
    for i in range(half - 1, slabs):
        for m in range(2):
            turn_slab(m, jnp.int32(i))
    for o in (1, 3, 2):
        spread(o).wait_recv()
    near = 2 - 2 * lax.rem(x, 2)
    first = xh[...].astype(F32) + xhr[near].astype(F32)
    attn = first + (xhr[1].astype(F32) + xhr[2 - near].astype(F32))
    left = pl.ds(pl.multiple_of(far * unit, unit), unit)
    hst[far] = (res[:, left].astype(F32) + attn).astype(BF16)
    dispatch(2)
    dispatch(3)
    square = jnp.zeros((block, 1), F32)
    for i in range(nz):
        state = hst[i].astype(F32)
        square = square + jnp.sum(state * state, axis=-1, keepdims=True)
    scale = lax.rsqrt(square / d_model + EPS)
    by_position = jnp.sum(jnp.where(same, scale, 0.0), axis=0, keepdims=True)
    by_row = jnp.sum(jnp.where(picked, by_position, 0.0), axis=1, keepdims=True)
    grid = (2 * GCAP, cnt.shape[3])
    diagonal = lax.broadcasted_iota(jnp.int32, grid, 0) == lax.broadcasted_iota(jnp.int32, grid, 1)
    row_scale = jnp.sum(jnp.where(diagonal, by_row, 0.0), axis=0, keepdims=True)
    cnt[z, c] = jnp.where(line == 0, lead, jnp.where(line == 1, row_scale, info))
    to_sibling = send(cnt.at[z, c], cnt.at[z, c], c0_s.at[0], c0_r.at[0], sibling)
    to_sibling.start()
    launch(2)
    launch(3)
    send(cnt.at[z, 1 - c], cnt.at[z, 1 - c], c0_s.at[0], c0_r.at[0], sibling).wait_recv()
    count_ring(1, z).start()
    for load in loads[5:]:
        load.wait()
    unit_rows = 2 * GCAP
    ffw = wg.shape[2]
    quarter = width // SUBS

    def arrive_count(s, last):
        u = unit_at(-s)
        count_ring(s, u).wait_recv()
        if not last:
            count_ring(s + 1, u).start()
            count_pair(s, u).start()

    def gate_up(j, units, first):
        slab = pl.ds(j * width, width) if isinstance(j, int) else pl.ds(
            pl.multiple_of(j * width, width), width
        )
        block_rows = jnp.concatenate([rows[u, j] for u in units], axis=0)
        many = len(units) * unit_rows
        for i in range(4):
            weight = (wg, wu)[i // 2]
            total = dot(block_rows, weight[i % 2, slab, :])
            if first:
                acc[i, :many] = total
            else:
                acc[i, :many] += total

    def activate(slot, units):
        many = len(units) * unit_rows
        row = lax.broadcasted_iota(jnp.int32, (many, ffw), 0).astype(F32)
        limit = cnt[units[0], 0, 0:1, 0:1]
        place = row
        for i in range(1, 2 * len(units)):
            later = row >= i * GCAP
            limit = jnp.where(later, cnt[units[i // 2], i % 2, 0:1, 0:1], limit)
            place = jnp.where(later, row - i * GCAP, place)
        second = place >= limit
        wide = (many, cnt.shape[3])
        at = lax.broadcasted_iota(jnp.int32, wide, 0) - lax.broadcasted_iota(jnp.int32, wide, 1)
        factor = jnp.zeros(wide, F32)
        for i, u in enumerate(units):
            row_scale = cnt[u, 0, 1:2, :] + cnt[u, 1, 1:2, :]
            factor = factor + jnp.where(at == i * unit_rows, row_scale, 0.0)
        factor = jnp.sum(factor, axis=1, keepdims=True)
        for e in range(2):
            g, up = acc[e, :many] * factor, acc[2 + e, :many] * factor
            value = g / (1.0 + jnp.exp(-g)) * up
            mine = second if e == 1 else jnp.logical_not(second)
            hid[slot, e, :many] = jnp.where(mine, value, 0.0).astype(BF16)

    def down(slot, f, units):
        many = len(units) * unit_rows
        for i in range(SUBS):
            start = f * width + i * quarter
            if not isinstance(f, int):
                start = pl.multiple_of(start, quarter)
            cols = pl.ds(start, quarter)
            total = dot(hid[slot, 0, :many], wd[0, :, cols]) + dot(hid[slot, 1, :many], wd[1, :, cols])
            for n, u in enumerate(units):
                part[u, f, :, i * quarter : (i + 1) * quarter] = total[
                    n * unit_rows : (n + 1) * unit_rows
                ].astype(BF16)

    def both(s):
        return (unit_at(-s), unit_at(s))

    def prepare(s, last=False):
        u = unit_at(s)
        for o in (1, 3, 2, 0):
            f = quarter_at(o)
            give(s, f, u).wait_recv()
            dbuf[s - 1, f] = (part[u, f].astype(F32) + dbuf[s - 1, f].astype(F32)).astype(BF16)
            if o in (1, 3):
                (over_far(o) if last else over(s, o, dbuf.at[s - 1, f])).start()

    def by_positions(s, mine, last=False):
        for o in (1, 3):
            (over_far(o) if last else over(s, o, xin.at[s, 0])).wait_recv()
        u = unit_at(s)
        facts = cnt[u, 0] + cnt[u, 1]
        row = lax.broadcasted_iota(jnp.int32, (unit_rows, cnt.shape[3]), 0).astype(F32) + 1.0
        highs, lows = [], []
        for i in range(3):
            hit = [row == facts[2 + 2 * i + k : 3 + 2 * i + k] for k in range(2)]
            for kept, at in ((highs, 8), (lows, 10)):
                kept.append(
                    jnp.where(hit[0], facts[at : at + 1], 0.0)
                    + jnp.where(hit[1], facts[at + 1 : at + 2], 0.0)
                )
        sums = jnp.concatenate([mine, xin[s, 0], xin[s, 1]], axis=0)
        total = None
        for weight in (highs, lows):
            turned = jnp.transpose(jnp.concatenate(weight, axis=0)).astype(BF16)
            term = dot(turned, sums)
            total = term if total is None else total + term
        return total

    def gather_positions(s, last=False):
        total = by_positions(s, dbuf[s - 1, x], last)
        for b in range(2):
            pos[s - 1, b] = total[b * block : (b + 1) * block].astype(BF16)

    def sum_p(t, b, arrived):
        if arrived:
            ring_p(t - 1, b).wait_recv()
            at = half - t - 1
            pos[at, b] = (pos[at, b].astype(F32) + posr[t - 1, b].astype(F32)).astype(BF16)
        ring_p(t, b).start()

    def sum_z(t, h, arrived):
        if arrived:
            ring_z(t - 1, h).wait_recv()
            at = half - t - 1
            f = quarter_at(2)
            dbuf[at, f, :, lanes(h)] = (
                dbuf[at, f, :, lanes(h)].astype(F32) + zsr[t - 1, h].astype(F32)
            ).astype(BF16)
        ring_z(t, h).start()

    def expert_step(s, carry):
        u = unit_at(-s)
        for k in range(SUBS):
            j = rows_at(u, k)
            ring2(s, j, u).wait_recv()

            @pl.when((s < half - 1) | (c == 1 if k < 2 else c == 0))
            def _():
                ring2(s + 1, j, u).start()

            pair2(s, j, u).start()
            if k == 2:
                arrive_count(s, False)
            @pl.when(s >= 2)
            def _():
                pair2(s - 1, k, unit_at(s - 1)).wait_recv()

            gate_up(k, both(s - 1), k == 0)
            if k == SUBS - 1:
                @pl.when(s >= 2)
                def _():
                    count_pair(s - 1, unit_at(s - 1)).wait_recv()

                activate(lax.rem(s - 1, 3), both(s - 1))

            @pl.when(s >= 2)
            def _():
                down(lax.rem(s - 2, 3), k, both(s - 2))

            @pl.when(s >= 3)
            def _():
                give(s - 2, k, unit_at(2 - s)).start()

        @pl.when(s == 3)
        def _():
            for o in (1, 3):
                over(0, o, part.at[z, quarter_at(o)]).start()

        @pl.when(s >= 4)
        def _():
            prepare(s - 3)

        return carry

    lax.fori_loop(1, half, expert_step, 0)

    own_far = [rows_at(far, 2 * (1 - c) + i) for i in range(2)]
    other_far = [rows_at(far, 2 * c + i) for i in range(2)]
    prepare(half - 3)
    for k in range(SUBS):
        pair2(half - 1, k, unit_at(half - 1)).wait_recv()
        if k == SUBS - 1:
            ring2(half, own_far[0], far).wait_recv()
            pair2(half, own_far[0], far).start()
        gate_up(k, both(half - 1), k == 0)
    count_pair(half - 1, unit_at(half - 1)).wait_recv()
    activate((half - 1) % 3, both(half - 1))
    for o in (1, 3, 2, 0):
        down((half - 1) % 3, quarter_at(o), both(half - 1))
        give(half - 1, quarter_at(o), unit_at(1 - half)).start()
    ring2(half, own_far[1], far).wait_recv()
    pair2(half, own_far[1], far).start()
    arrive_count(half, True)

    prepare(half - 1)
    sum_z(1, 1 - c, False)
    single = (far,)
    for i in range(2):
        gate_up(own_far[i], single, i == 0)
    for i in range(2):
        pair2(half, other_far[i], far).wait_recv()
        gate_up(other_far[i], single, False)
    activate(half % 3, single)
    for o in (1, 3, 2, 0):
        down(half % 3, quarter_at(o), single)
        give(half, quarter_at(o), far).start()
    prepare(half, True)
    sum_z(0, c, False)
    gather_positions(half - 1)
    sum_p(1, 1 - c, False)
    for o in (1, 3, 2, 0):
        down((half - 2) % 3, quarter_at(o), both(half - 2))
        give(half - 2, quarter_at(o), unit_at(2 - half)).start()
    prepare(half - 2)
    sum_z(2, 1 - c, True)
    gather_positions(half, True)
    sum_p(0, c, False)
    sum_z(1, c, True)
    total = by_positions(0, part[z, x])
    for b in range(2):
        base[b] = total[b * block : (b + 1) * block]

    def sum_step(t, carry):
        @pl.when(t < half)
        def _():
            sum_z(t, 1 - c, True)

        sum_z(t - 1, c, True)
        sum_p(t - 2, c, True)
        gather_positions(half - t + 1)
        sum_p(t - 1, 1 - c, True)
        return carry

    lax.fori_loop(3, half + 1, sum_step, 0)

    def swap_z(h):
        return send(finz.at[h], finzr.at[h], fi_s.at[h], fi_r.at[h], sibling)

    swap_p = send(finp, finpr, fi_s.at[2], fi_r.at[2], sibling)

    def close_z(h):
        ring_z(half - 1, h).wait_recv()
        own_part = part[z, quarter_at(2), :, lanes(h)]
        finz[h] = (own_part.astype(F32) + zsr[half - 1, h].astype(F32)).astype(BF16)
        swap_z(h).start()

    def deliver(h):
        return send(con.at[h], conr.at[h], co_s.at[h], co_r.at[h], x_other[2])

    def cross(h):
        swap_z(h).wait_recv()
        total = (finz[h].astype(F32) + finzr[h].astype(F32)).astype(BF16)
        con[h] = (dot(mix[0], total) + dot(mix[1], total)).astype(BF16)
        deliver(h).start()

    close_z(1 - c)
    close_z(c)
    cross(0)
    cross(1)
    sum_p(half - 1, c, True)
    ring_p(half - 1, 1 - c).wait_recv()
    finp[...] = (base[1 - c] + posr[half - 1, 1 - c].astype(F32)).astype(BF16)
    swap_p.start()
    ring_p(half - 1, c).wait_recv()
    swap_p.wait_recv()
    base[c] = base[c] + posr[half - 1, c].astype(F32) + finpr[...].astype(F32)
    for h in range(2):
        deliver(h).wait_recv()
        for i in range(half_width // min(unit, half_width)):
            step = min(unit, half_width)
            at = h * half_width + i * step
            state = hst[x * per_sub + at // unit][:, at % unit : at % unit + step]
            total = state.astype(F32) + base[c, :, at : at + step]
            total = total + conr[h, :, i * step : (i + 1) * step].astype(F32)
            out_ref[:, at : at + step] = total.astype(BF16)
    for i in range(2):
        send(ow.at[z, i], ow.at[z, i], d0_s.at[i], d0_r.at[i], sibling).wait_send()
    to_sibling.wait_send()

    def drain(s, carry):
        count_ring(s, z).wait_send()
        swap_a(s - 1).wait_send()
        swap_b(s - 1).wait_send()
        for j in range(SUBS):
            @pl.when(s < half)
            def _():
                for make in (ring1, ring2, pair1, pair2):
                    make(s, j, z).wait_send()

            give(s, j, z).wait_send()

        @pl.when(s < half)
        def _():
            for o in (1, 3):
                over(s, o, xin.at[s, 0]).wait_send()
            count_pair(s, z).wait_send()
            for b in range(2):
                ring_p(s, b).wait_send()
                ring_z(s, b).wait_send()

        return carry

    lax.fori_loop(1, half + 1, drain, 0)
    for k in range(2):
        j = sub_at(k)
        for make in (ring1, pair1):
            make(half, j, z).wait_send()
        ring2(half, rows_at(unit_at(1 - half), 2 * (1 - c) + k), z).wait_send()
        pair2(half, own_far[k], z).wait_send()
        deliver(k).wait_send()
        swap_z(k).wait_send()
        over(0, 1 + 2 * k, xin.at[0, 0]).wait_send()
        over_far(1 + 2 * k).wait_send()
    for j in range(SUBS):
        send(own.at[j], oth.at[j], ot_s.at[j], ot_r.at[j], sibling).wait_send()
    for o in (1, 2, 3):
        spread(o).wait_send()
    ring_p(0, c).wait_send()
    ring_z(0, c).wait_send()
    swap_p.wait_send()


def per_device(nz, *args):
    (queries, keys, values, out_weight, residual, gain, ids, slots, weights, w_gate, w_up, w_down) = args
    block, heads_width = queries.shape
    d_model = residual.shape[1]
    width = d_model // SUBS
    half = nz // 2
    lane = out_weight.shape[1]
    ow_rows = out_weight.shape[0] // 2
    unit_rows = 2 * GCAP
    ffw = w_gate.shape[2]
    w_gate, w_up = (jnp.swapaxes(w, 1, 2) for w in (w_gate, w_up))
    vmem = pl.BlockSpec(memory_space=pltpu.VMEM)
    hbm = pl.BlockSpec(memory_space=pl.ANY)
    dma = pltpu.SemaphoreType.DMA
    swap = pltpu.VMEM((half, block, 4 * lane), BF16)
    sub = pltpu.VMEM((SUBS, unit_rows, width), BF16)
    scratch = [
        pltpu.VMEM(keys.shape[1:], BF16),
        pltpu.VMEM(values.shape[1:], BF16),
        pltpu.VMEM(residual.shape, BF16),
        pltpu.VMEM((2, d_model, ffw), BF16),
        pltpu.VMEM((2, d_model, ffw), BF16),
        pltpu.VMEM(w_down.shape, BF16),
        pltpu.VMEM((2, 2, ffw, width), BF16),
        pltpu.VMEM((block, heads_width), BF16),
        pltpu.VMEM((nz, SUBS, ow_rows, lane), BF16),
        swap,
        swap,
        swap,
        swap,
        pltpu.VMEM((nz, block, 2 * lane), BF16),
        sub,
        sub,
        pltpu.VMEM((nz, SUBS, unit_rows, width), BF16),
        pltpu.VMEM((nz, 2, 16, 128), F32),
        pltpu.VMEM((4, 2 * unit_rows, ffw), F32),
        pltpu.VMEM((3, 2, 2 * unit_rows, ffw), BF16),
        pltpu.VMEM((nz, SUBS, unit_rows, width), BF16),
        pltpu.VMEM((half, SUBS, unit_rows, width), BF16),
        pltpu.VMEM((half + 1, 2, unit_rows, width), BF16),
        pltpu.VMEM((half, 2, block, width), BF16),
        pltpu.VMEM((half, 2, block, width), BF16),
        pltpu.VMEM((half, 2, unit_rows, width // 2), BF16),
        pltpu.VMEM((2, block, width), F32),
        *[pltpu.VMEM((block, width), BF16)] * 2,
        *[pltpu.VMEM((2, unit_rows, width // 2), BF16)] * 2,
        *[pltpu.VMEM((2, block, width // 2), BF16)] * 2,
        pltpu.VMEM((block, 2 * lane), BF16),
        pltpu.VMEM((3, block, 2 * lane), BF16),
        pltpu.VMEM((2, block, unit_rows), BF16),
        dma((6,)),
        dma((2, 2)),
        dma((2,)),
        dma((2,)),
        *[dma((half + 1, SUBS))] * 4,
        *[dma((half,))] * 4,
        *[dma((SUBS,))] * 2,
        *[dma((half + 1, SUBS))] * 4,
        *[dma((1,))] * 2,
        *[dma((half + 1,))] * 4,
        *[dma((half, SUBS))] * 2,
        *[dma((half + 1, 2))] * 2,
        *[dma((half, SUBS))] * 2,
        *[dma((3,))] * 2,
        *[dma((2,))] * 2,
        *[dma((3,))] * 2,
    ]
    return pl.pallas_call(
        functools.partial(layer_kernel, nz),
        out_shape=jax.ShapeDtypeStruct((block, width), BF16),
        in_specs=[vmem, hbm, hbm, hbm, hbm, vmem, vmem, vmem, vmem, hbm, hbm, hbm],
        out_specs=vmem,
        scratch_shapes=scratch,
        compiler_params=pltpu.CompilerParams(
            collective_id=0, has_side_effects=True, vmem_limit_bytes=67043328
        ),
    )(queries, keys, values, out_weight, residual, gain.reshape(1, -1), ids.T, slots.T, weights.T, w_gate, w_up, w_down)


def solution(mesh):
    in_specs = (
        P(("groups", "fsdp"), "expert"),
        P(("groups", "fsdp"), None, "expert"),
        P(("groups", "fsdp"), None, "expert"),
        P("expert", "fsdp"),
        P(("groups", "fsdp"), None),
        P(),
        P(("groups", "fsdp"), None),
        P(("groups", "fsdp"), None),
        P(("groups", "fsdp"), None),
        P("expert", None, "fsdp"),
        P("expert", None, "fsdp"),
        P("expert", "fsdp", None),
    )
    return jax.shard_map(
        functools.partial(per_device, mesh.shape["fsdp"] // 2),
        mesh=mesh,
        in_specs=in_specs,
        out_specs=P(("groups", "fsdp"), "expert"),
        check_vma=False,
    )
```

```python
import functools

import jax
import jax.numpy as jnp
from jax import lax
from jax.experimental import pallas as pl
from jax.experimental.pallas import tpu as pltpu
from jax.sharding import PartitionSpec as P

HEAD_DIM = 128
GCAP = 36
SUBS = 4
EPS = 1e-05
MESH = pl.DeviceIdType.MESH
F32 = jnp.float32
BF16 = jnp.bfloat16


def dot(a, b):
    return jnp.dot(a, b, preferred_element_type=F32)


def layer_kernel(
    nz,
    q_ref,
    k_hbm,
    v_hbm,
    ow_hbm,
    res_hbm,
    gain_ref,
    ids_ref,
    slots_ref,
    weights_ref,
    wg_hbm,
    wu_hbm,
    wd_hbm,
    out_ref,
    keys,
    vals,
    res,
    wg,
    wu,
    wd,
    stage,
    heads,
    ow,
    xa,
    xar,
    xb,
    xbr,
    hst,
    own,
    oth,
    rows,
    cnt,
    acc,
    hid,
    part,
    dbuf,
    xin,
    pos,
    posr,
    zsr,
    base,
    finp,
    finpr,
    finz,
    finzr,
    con,
    conr,
    xh,
    xhr,
    mix,
    lsem,
    wsem,
    d0_s,
    d0_r,
    r1_s,
    r1_r,
    d1_s,
    d1_r,
    xa_s,
    xa_r,
    xb_s,
    xb_r,
    ot_s,
    ot_r,
    r2_s,
    r2_r,
    d2_s,
    d2_r,
    c0_s,
    c0_r,
    cr_s,
    cr_r,
    cd_s,
    cd_r,
    db_s,
    db_r,
    xi_s,
    xi_r,
    rs_s,
    rs_r,
    fi_s,
    fi_r,
    co_s,
    co_r,
    xh_s,
    xh_r,
):
    half = nz // 2
    half_width = zsr.shape[3]
    n2 = lax.axis_index("fsdp")
    c = lax.rem(n2, 2)
    z = n2 // 2
    x = lax.axis_index("expert")
    step_dir = 2 * c - 1
    ring_next = {"fsdp": lax.rem(z + step_dir + nz, nz) * 2 + c}
    ring_prev = {"fsdp": lax.rem(z - step_dir + nz, nz) * 2 + c}
    sibling = {"fsdp": z * 2 + 1 - c}
    x_first = {"expert": x + 1 - 2 * lax.rem(x, 2)}
    x_second = {"expert": 3 - x}
    x_other = [{"expert": lax.rem(x + o, 4)} for o in range(4)]

    def unit_at(s):
        return lax.rem(z + s * step_dir + 2 * nz, nz)

    def sub_at(k):
        return lax.rem(2 * c + k, SUBS)

    def send(src, dst, s_sem, r_sem, device):
        return pltpu.make_async_remote_copy(
            src_ref=src, dst_ref=dst, send_sem=s_sem, recv_sem=r_sem,
            device_id=device, device_id_type=MESH,
        )

    def ring1(s, j, u):
        ref = ow.at[u, j]
        return send(ref, ref, r1_s.at[s, j], r1_r.at[s, j], ring_next)

    def pair1(s, j, u):
        ref = ow.at[u, j]
        return send(ref, ref, d1_s.at[s, j], d1_r.at[s, j], sibling)

    def ring2(s, j, u):
        ref = rows.at[u, j]
        return send(ref, ref, r2_s.at[s, j], r2_r.at[s, j], ring_next)

    def pair2(s, j, u):
        ref = rows.at[u, j]
        return send(ref, ref, d2_s.at[s, j], d2_r.at[s, j], sibling)

    def count_ring(s, u):
        return send(cnt.at[u], cnt.at[u], cr_s.at[s], cr_r.at[s], ring_next)

    def count_pair(s, u):
        return send(cnt.at[u], cnt.at[u], cd_s.at[s], cd_r.at[s], sibling)

    def swap_a(s):
        return send(xa.at[s], xar.at[s], xa_s.at[s], xa_r.at[s], x_first)

    def swap_b(s):
        return send(xb.at[s], xbr.at[s], xb_s.at[s], xb_r.at[s], x_second)

    def give(s, j, u):
        return send(part.at[u, j], dbuf.at[s - 1, j], db_s.at[s - 1, j], db_r.at[s - 1, j], sibling)

    def quarter_at(o):
        return lax.rem(x + o, 4)

    def lanes(h):
        return pl.ds(pl.multiple_of(h * half_width, half_width), half_width)

    def ring_p(t, b, g):
        sems = rs_s.at[t, 2 * b + g], rs_r.at[t, 2 * b + g]
        cols = pl.ds(g * half_width, half_width)
        src = pos.at[half - t - 1, b, :, cols]
        return send(src, posr.at[t, b, :, cols], *sems, ring_next)

    def ring_z(t, h):
        sems = rs_s.at[t, 4 + h], rs_r.at[t, 4 + h]
        src = dbuf.at[half - t - 1, quarter_at(2), :, lanes(h)]
        return send(src, zsr.at[t, h], *sems, ring_next)

    def over_far(o):
        i = 1 if o == 1 else 0
        part_rows = pl.ds(pl.multiple_of(32 * c, 32), 40)
        src = dbuf.at[half - 1, quarter_at(o), part_rows]
        dst = xin.at[half, i, part_rows]
        return send(src, dst, xi_s.at[half, i], xi_r.at[half, i], x_other[o])

    def over(s, o, src):
        i = 1 if o == 1 else 0
        return send(src, xin.at[s, i], xi_s.at[s, i], xi_r.at[s, i], x_other[o])

    own_rows = ow_hbm.shape[0] // 2
    loads = [
        pltpu.make_async_copy(ow_hbm.at[pl.ds(0, own_rows)], ow.at[z, 2 * c], lsem.at[0]),
        pltpu.make_async_copy(ow_hbm.at[pl.ds(own_rows, own_rows)], ow.at[z, 2 * c + 1], lsem.at[1]),
        pltpu.make_async_copy(k_hbm.at[0], keys, lsem.at[2]),
        pltpu.make_async_copy(v_hbm.at[0], vals, lsem.at[3]),
        pltpu.make_async_copy(res_hbm, res, lsem.at[4]),
        pltpu.make_async_copy(wd_hbm, wd, lsem.at[5]),
    ]

    slabs = 2 * SUBS
    slab_width = stage.shape[3]

    def slab_load(m, i):
        cols = pl.ds(pl.multiple_of((i % SUBS) * slab_width, slab_width), slab_width)
        src = (wg_hbm, wu_hbm)[m].at[i // SUBS, :, cols]
        return pltpu.make_async_copy(src, stage.at[m, i % 2], wsem.at[m, i % 2])

    def turn_slab(m, i):
        slab_load(m, i).wait()
        at = pl.ds(pl.multiple_of((i % SUBS) * slab_width, slab_width), slab_width)
        (wg, wu)[m][i // SUBS, at, :] = jnp.transpose(stage[m, i % 2])

        @pl.when(i + 2 < slabs)
        def _():
            slab_load(m, i + 2).start()

    for load in loads[:5]:
        load.start()
    for i in range(2):
        for m in range(2):
            slab_load(m, jnp.int32(i)).start()
    loads[5].start()

    xin[half] = jnp.zeros(xin.shape[1:], BF16)
    barrier = pltpu.get_barrier_semaphore()
    partners = [ring_next, ring_prev, sibling, *x_other[1:]]
    for device in partners:
        pl.semaphore_signal(barrier, inc=1, device_id=device, device_id_type=MESH)
    pl.semaphore_wait(barrier, len(partners))

    loads[0].wait()
    loads[1].wait()
    for i in range(2):
        j = 2 * c + i
        send(ow.at[z, j], ow.at[z, j], d0_s.at[i], d0_r.at[i], sibling).start()
        ring1(1, j, z).start()
    for i in range(2):
        j = 2 * (1 - c) + i
        send(ow.at[z, j], ow.at[z, j], d0_s.at[i], d0_r.at[i], sibling).wait_recv()
        ring1(1, j, z).start()

    loads[2].wait()
    loads[3].wait()
    block, heads_width = q_ref.shape
    context = keys.shape[0]
    key_pos = lax.broadcasted_iota(jnp.int32, (block, context), 1)
    query_pos = context - block + lax.broadcasted_iota(jnp.int32, (block, context), 0)
    allowed = key_pos <= query_pos
    for h in range(heads_width // HEAD_DIM):
        cols = slice(h * HEAD_DIM, (h + 1) * HEAD_DIM)
        scores = lax.dot_general(
            q_ref[:, cols], keys[...], (((1,), (1,)), ((), ())), preferred_element_type=F32
        ) * HEAD_DIM ** (-0.5)
        masked = jnp.where(allowed, scores, -1e30)
        highest = jnp.max(masked, axis=-1, keepdims=True)
        weights = jnp.where(allowed, jnp.exp(masked - highest), 0.0)
        probs = (weights / jnp.sum(weights, axis=-1, keepdims=True)).astype(BF16)
        heads[:, cols] = dot(probs, vals[...]).astype(BF16)

    unit = 2 * ow.shape[3]
    lane = ow.shape[3]

    def project(s):
        for side, u in enumerate((unit_at(-s), unit_at(s))):
            for b in range(2):
                total = dot(heads[:, :own_rows], ow[u, 2 * b]) + dot(
                    heads[:, own_rows:], ow[u, 2 * b + 1]
                )
                at = side * unit + b * lane
                xa[s, :, at : at + lane] = total.astype(BF16)
        swap_a(s).start()

    def add_first(s):
        swap_a(s).wait_recv()
        xb[s] = (xa[s].astype(F32) + xar[s].astype(F32)).astype(BF16)
        swap_b(s).start()

    def add_second(s):
        swap_b(s).wait_recv()
        for side, u in enumerate((unit_at(-s), unit_at(s))):
            cols = slice(side * unit, (side + 1) * unit)
            attn = xb[s, :, cols].astype(F32) + xbr[s, :, cols].astype(F32)
            left = pl.ds(pl.multiple_of(u * unit, unit), unit)
            hst[u] = (res[:, left].astype(F32) + attn).astype(BF16)

    first_expert = 2 * x
    ids = ids_ref[...]
    within = ids - first_expert
    in_group = (within >= 0) & (within < 2)
    is_first = jnp.where(ids == first_expert, 1.0, 0.0)
    lead = jnp.sum(jnp.sum(is_first, axis=1, keepdims=True), axis=0, keepdims=True)
    target = jnp.where(in_group, slots_ref[...] + within * lead.astype(jnp.int32) + GCAP * c, -1)
    row_ids = lax.broadcasted_iota(jnp.int32, (2 * GCAP, block), 0)
    picks = [row_ids == target[k : k + 1, :] for k in range(2)]
    picked = picks[0] | picks[1]
    one_hot = jnp.where(picked, 1.0, 0.0).astype(BF16)
    share = weights_ref[...].astype(F32) / 65536.0
    share_high = share.astype(BF16).astype(F32)
    facts = [share_high[0:1], share_high[1:2], share[0:1] - share_high[0:1], share[1:2] - share_high[1:2]]
    for o in (3, 1, 0):
        other = 2 * lax.rem(x + o, 4)
        inside = (ids >= other) & (ids < other + 2)
        count = jnp.where(ids == other, 1.0, 0.0)
        count = jnp.sum(jnp.sum(count, axis=1, keepdims=True), axis=0, keepdims=True)
        place = slots_ref[...] + (ids - other) * count.astype(jnp.int32) + GCAP * c + 1
        place = jnp.where(inside, place, 0).astype(F32)
        facts = [place[0:1], place[1:2]] + facts
    shift = (block, cnt.shape[3])
    spot = lax.broadcasted_iota(jnp.int32, shift, 0) + block * c
    placed = spot == lax.broadcasted_iota(jnp.int32, shift, 1)
    same = (
        lax.broadcasted_iota(jnp.int32, (block, block), 0)
        == lax.broadcasted_iota(jnp.int32, (block, block), 1)
    )
    line = lax.broadcasted_iota(jnp.int32, cnt.shape[2:], 0)
    info = jnp.zeros(cnt.shape[2:], F32)
    for i, fact in enumerate(facts):
        column = jnp.sum(jnp.where(same, fact, 0.0), axis=1, keepdims=True)
        wide_fact = jnp.sum(jnp.where(placed, column, 0.0), axis=0, keepdims=True)
        info = jnp.where(line == i + 2, wide_fact, info)
    mixed = jnp.where(picks[0], share[0:1, :], 0.0) + jnp.where(picks[1], share[1:2, :], 0.0)
    high = mixed.astype(BF16)
    low = (mixed - high.astype(F32)).astype(BF16)
    turn = jnp.where(same, 1.0, 0.0).astype(BF16)
    for i, piece in enumerate((high, low)):
        mix[i] = lax.dot_general(
            turn, piece, (((1,), (1,)), ((), ())), preferred_element_type=F32
        ).astype(BF16)
    loads[4].wait()

    def take_pair(s):
        for j in range(SUBS):
            pair1(s, j, unit_at(s)).wait_recv()

    def projection_step(s, carry):
        u = unit_at(-s)
        for k in range(SUBS):
            j = sub_at(k)
            ring1(s, j, u).wait_recv()
            if k < 2:
                ring1(s + 1, j, u).start()
            else:
                @pl.when(s < half - 1)
                def _():
                    ring1(s + 1, j, u).start()
            pair1(s, j, u).start()
            if k in (0, 2):
                turn_slab(k // 2, s - 1)
            if k == 1:
                @pl.when(s >= 2)
                def _():
                    take_pair(s - 1)

                project(s - 1)

                @pl.when(s >= 2)
                def _():
                    add_first(s - 2)

                @pl.when(s >= 3)
                def _():
                    add_second(s - 3)

        return carry

    lax.fori_loop(1, half, projection_step, 0)
    u = unit_at(half)
    ring1(half, sub_at(0), u).wait_recv()
    pair1(half, sub_at(0), u).start()
    take_pair(half - 1)
    project(half - 1)
    ring1(half, sub_at(1), u).wait_recv()
    pair1(half, sub_at(1), u).start()
    add_first(half - 2)
    if half >= 3:
        add_second(half - 3)
    width = rows.shape[3]
    per_sub = width // unit
    d_model = width * SUBS

    def rows_at(u, k):
        return lax.rem(lax.rem(u + half + 1, nz) // per_sub + 1 + k, SUBS)

    def trade(j):
        return send(own.at[j], oth.at[j], ot_s.at[j], ot_r.at[j], sibling)

    def dispatch(k):
        j = rows_at(z, k)
        for i in range(per_sub):
            u = j * per_sub + i
            gain = gain_ref[:, pl.ds(pl.multiple_of(u * unit, unit), unit)]
            scaled = (hst[u].astype(F32) * gain).astype(BF16)
            own[j, :, i * unit : (i + 1) * unit] = dot(one_hot, scaled).astype(BF16)
        trade(j).start()

    def launch(k):
        j = rows_at(z, k)
        trade(j).wait_recv()
        rows[z, j] = own[j] + oth[j]
        ring2(1, j, z).start()

    far = unit_at(half)
    for k in range(2, 4):
        pair1(half, sub_at(k), far).wait_recv()
    for b in range(2):
        total = dot(heads[:, :own_rows], ow[far, 2 * b]) + dot(
            heads[:, own_rows:], ow[far, 2 * b + 1]
        )
        xh[:, b * lane : (b + 1) * lane] = total.astype(BF16)

    def spread(o):
        return send(xh, xhr.at[o - 1], xh_s.at[o - 1], xh_r.at[o - 1], x_other[o])

    for o in (2, 1, 3):
        spread(o).start()
    add_first(half - 1)
    add_second(half - 2)
    dispatch(0)
    dispatch(1)
    launch(0)
    launch(1)
    add_second(half - 1)
    for i in range(half - 1, slabs):
        for m in range(2):
            turn_slab(m, jnp.int32(i))
    for o in (1, 3, 2):
        spread(o).wait_recv()
    near = 2 - 2 * lax.rem(x, 2)
    first = xh[...].astype(F32) + xhr[near].astype(F32)
    attn = first + (xhr[1].astype(F32) + xhr[2 - near].astype(F32))
    left = pl.ds(pl.multiple_of(far * unit, unit), unit)
    hst[far] = (res[:, left].astype(F32) + attn).astype(BF16)
    dispatch(2)
    dispatch(3)
    square = jnp.zeros((block, 1), F32)
    for i in range(nz):
        state = hst[i].astype(F32)
        square = square + jnp.sum(state * state, axis=-1, keepdims=True)
    scale = lax.rsqrt(square / d_model + EPS)
    by_position = jnp.sum(jnp.where(same, scale, 0.0), axis=0, keepdims=True)
    by_row = jnp.sum(jnp.where(picked, by_position, 0.0), axis=1, keepdims=True)
    grid = (2 * GCAP, cnt.shape[3])
    diagonal = lax.broadcasted_iota(jnp.int32, grid, 0) == lax.broadcasted_iota(jnp.int32, grid, 1)
    row_scale = jnp.sum(jnp.where(diagonal, by_row, 0.0), axis=0, keepdims=True)
    scale_high = row_scale.astype(BF16).astype(F32)
    info = jnp.where(line == 12, row_scale - scale_high, info)
    cnt[z, c] = jnp.where(line == 0, lead, jnp.where(line == 1, scale_high, info)).astype(BF16)
    to_sibling = send(cnt.at[z, c], cnt.at[z, c], c0_s.at[0], c0_r.at[0], sibling)
    to_sibling.start()
    launch(2)
    launch(3)
    send(cnt.at[z, 1 - c], cnt.at[z, 1 - c], c0_s.at[0], c0_r.at[0], sibling).wait_recv()
    count_ring(1, z).start()
    for load in loads[5:]:
        load.wait()
    unit_rows = 2 * GCAP
    ffw = wg.shape[2]
    quarter = width // SUBS

    def arrive_count(s, last):
        u = unit_at(-s)
        count_ring(s, u).wait_recv()
        if not last:
            count_ring(s + 1, u).start()
            count_pair(s, u).start()

    def gate_up(j, units, first):
        slab = pl.ds(j * width, width) if isinstance(j, int) else pl.ds(
            pl.multiple_of(j * width, width), width
        )
        block_rows = jnp.concatenate([rows[u, j] for u in units], axis=0)
        many = len(units) * unit_rows
        for i in range(4):
            weight = (wg, wu)[i // 2]
            total = dot(block_rows, weight[i % 2, slab, :])
            if first:
                acc[i, :many] = total
            else:
                acc[i, :many] += total

    def activate(slot, units):
        many = len(units) * unit_rows
        row = lax.broadcasted_iota(jnp.int32, (many, ffw), 0).astype(F32)
        facts = [[cnt[u, b].astype(F32) for b in range(2)] for u in units]
        limit = facts[0][0][0:1, 0:1]
        place = row
        for i in range(1, 2 * len(units)):
            later = row >= i * GCAP
            limit = jnp.where(later, facts[i // 2][i % 2][0:1, 0:1], limit)
            place = jnp.where(later, row - i * GCAP, place)
        second = place >= limit
        wide = (many, cnt.shape[3])
        at = lax.broadcasted_iota(jnp.int32, wide, 0) - lax.broadcasted_iota(jnp.int32, wide, 1)
        factor = jnp.zeros(wide, F32)
        for i, u in enumerate(units):
            known = facts[i][0] + facts[i][1]
            row_scale = known[1:2] + known[12:13]
            factor = factor + jnp.where(at == i * unit_rows, row_scale, 0.0)
        factor = jnp.sum(factor, axis=1, keepdims=True)
        for e in range(2):
            g, up = acc[e, :many] * factor, acc[2 + e, :many] * factor
            value = g / (1.0 + jnp.exp(-g)) * up
            mine = second if e == 1 else jnp.logical_not(second)
            hid[slot, e, :many] = jnp.where(mine, value, 0.0).astype(BF16)

    def down(slot, f, units):
        many = len(units) * unit_rows
        for i in range(SUBS):
            start = f * width + i * quarter
            if not isinstance(f, int):
                start = pl.multiple_of(start, quarter)
            cols = pl.ds(start, quarter)
            total = dot(hid[slot, 0, :many], wd[0, :, cols]) + dot(hid[slot, 1, :many], wd[1, :, cols])
            for n, u in enumerate(units):
                part[u, f, :, i * quarter : (i + 1) * quarter] = total[
                    n * unit_rows : (n + 1) * unit_rows
                ].astype(BF16)

    def both(s):
        return (unit_at(-s), unit_at(s))

    def prepare(s, last=False):
        u = unit_at(s)
        for o in (1, 3, 2, 0):
            f = quarter_at(o)
            give(s, f, u).wait_recv()
            dbuf[s - 1, f] = (part[u, f].astype(F32) + dbuf[s - 1, f].astype(F32)).astype(BF16)
            if o in (1, 3):
                (over_far(o) if last else over(s, o, dbuf.at[s - 1, f])).start()

    def by_positions(s, mine, last=False):
        for o in (1, 3):
            (over_far(o) if last else over(s, o, xin.at[s, 0])).wait_recv()
        u = unit_at(s)
        facts = cnt[u, 0].astype(F32) + cnt[u, 1].astype(F32)
        row = lax.broadcasted_iota(jnp.int32, (unit_rows, cnt.shape[3]), 0).astype(F32) + 1.0
        highs, lows = [], []
        for i in range(3):
            hit = [row == facts[2 + 2 * i + k : 3 + 2 * i + k] for k in range(2)]
            for kept, at in ((highs, 8), (lows, 10)):
                kept.append(
                    jnp.where(hit[0], facts[at : at + 1], 0.0)
                    + jnp.where(hit[1], facts[at + 1 : at + 2], 0.0)
                )
        sums = jnp.concatenate([mine, xin[s, 0], xin[s, 1]], axis=0)
        total = None
        for weight in (highs, lows):
            turned = jnp.transpose(jnp.concatenate(weight, axis=0)).astype(BF16)
            term = dot(turned, sums)
            total = term if total is None else total + term
        return total

    def gather_positions(s, last=False):
        total = by_positions(s, dbuf[s - 1, x], last)
        for b in range(2):
            pos[s - 1, b] = total[b * block : (b + 1) * block].astype(BF16)

    def sum_p(t, b, arrived):
        at = half - t - 1
        for g in range(2):
            if arrived:
                ring_p(t - 1, b, g).wait_recv()
                cols = slice(g * half_width, (g + 1) * half_width)
                total = pos[at, b, :, cols].astype(F32) + posr[t - 1, b, :, cols].astype(F32)
                pos[at, b, :, cols] = total.astype(BF16)
            ring_p(t, b, g).start()

    def sum_z(t, h, arrived):
        if arrived:
            ring_z(t - 1, h).wait_recv()
            at = half - t - 1
            f = quarter_at(2)
            dbuf[at, f, :, lanes(h)] = (
                dbuf[at, f, :, lanes(h)].astype(F32) + zsr[t - 1, h].astype(F32)
            ).astype(BF16)
        ring_z(t, h).start()

    def expert_step(s, carry):
        u = unit_at(-s)
        for k in range(SUBS):
            j = rows_at(u, k)
            ring2(s, j, u).wait_recv()

            @pl.when((s < half - 1) | (c == 1 if k < 2 else c == 0))
            def _():
                ring2(s + 1, j, u).start()

            pair2(s, j, u).start()
            if k == 2:
                arrive_count(s, False)
            @pl.when(s >= 2)
            def _():
                pair2(s - 1, k, unit_at(s - 1)).wait_recv()

            gate_up(k, both(s - 1), k == 0)
            if k == SUBS - 1:
                @pl.when(s >= 2)
                def _():
                    count_pair(s - 1, unit_at(s - 1)).wait_recv()

                activate(lax.rem(s - 1, 3), both(s - 1))

            @pl.when(s >= 2)
            def _():
                down(lax.rem(s - 2, 3), k, both(s - 2))

            @pl.when(s >= 3)
            def _():
                give(s - 2, k, unit_at(2 - s)).start()

        @pl.when(s == 3)
        def _():
            for o in (1, 3):
                over(0, o, part.at[z, quarter_at(o)]).start()

        @pl.when(s >= 4)
        def _():
            prepare(s - 3)

        return carry

    lax.fori_loop(1, half, expert_step, 0)

    own_far = [rows_at(far, 2 * (1 - c) + i) for i in range(2)]
    other_far = [rows_at(far, 2 * c + i) for i in range(2)]
    prepare(half - 3)
    for k in range(SUBS):
        pair2(half - 1, k, unit_at(half - 1)).wait_recv()
        if k == SUBS - 1:
            ring2(half, own_far[0], far).wait_recv()
            pair2(half, own_far[0], far).start()
        gate_up(k, both(half - 1), k == 0)
    count_pair(half - 1, unit_at(half - 1)).wait_recv()
    activate((half - 1) % 3, both(half - 1))
    for o in (1, 3, 2, 0):
        down((half - 1) % 3, quarter_at(o), both(half - 1))
        give(half - 1, quarter_at(o), unit_at(1 - half)).start()
    ring2(half, own_far[1], far).wait_recv()
    pair2(half, own_far[1], far).start()
    arrive_count(half, True)

    prepare(half - 1)
    sum_z(1, 1 - c, False)
    single = (far,)
    for i in range(2):
        gate_up(own_far[i], single, i == 0)
    for i in range(2):
        pair2(half, other_far[i], far).wait_recv()
        gate_up(other_far[i], single, False)
    activate(half % 3, single)
    for o in (1, 3, 2, 0):
        down(half % 3, quarter_at(o), single)
        give(half, quarter_at(o), far).start()
    for o in (1, 3, 2, 0):
        down((half - 2) % 3, quarter_at(o), both(half - 2))
        give(half - 2, quarter_at(o), unit_at(2 - half)).start()
    prepare(half, True)
    sum_z(0, c, False)
    gather_positions(half - 1)
    sum_p(1, 1 - c, False)
    prepare(half - 2)
    sum_z(2, 1 - c, True)
    gather_positions(half, True)
    sum_p(0, c, False)
    sum_z(1, c, True)
    total = by_positions(0, part[z, x])
    for b in range(2):
        base[b] = total[b * block : (b + 1) * block]

    def sum_step(t, carry):
        @pl.when(t < half)
        def _():
            sum_z(t, 1 - c, True)

        sum_z(t - 1, c, True)
        sum_p(t - 2, c, True)
        gather_positions(half - t + 1)
        sum_p(t - 1, 1 - c, True)
        return carry

    lax.fori_loop(3, half + 1, sum_step, 0)

    def swap_z(h):
        return send(finz.at[h], finzr.at[h], fi_s.at[h], fi_r.at[h], sibling)

    swap_p = send(finp, finpr, fi_s.at[2], fi_r.at[2], sibling)

    def close_z(h):
        ring_z(half - 1, h).wait_recv()
        own_part = part[z, quarter_at(2), :, lanes(h)]
        finz[h] = (own_part.astype(F32) + zsr[half - 1, h].astype(F32)).astype(BF16)
        swap_z(h).start()

    def deliver(h):
        return send(con.at[h], conr.at[h], co_s.at[h], co_r.at[h], x_other[2])

    def cross(h):
        swap_z(h).wait_recv()
        total = (finz[h].astype(F32) + finzr[h].astype(F32)).astype(BF16)
        con[h] = (dot(mix[0], total) + dot(mix[1], total)).astype(BF16)
        deliver(h).start()

    close_z(1 - c)
    close_z(c)
    cross(0)
    cross(1)
    sum_p(half - 1, c, True)
    for g in range(2):
        ring_p(half - 1, 1 - c, g).wait_recv()
    finp[...] = (base[1 - c] + posr[half - 1, 1 - c].astype(F32)).astype(BF16)
    swap_p.start()
    for g in range(2):
        ring_p(half - 1, c, g).wait_recv()
    swap_p.wait_recv()
    base[c] = base[c] + posr[half - 1, c].astype(F32) + finpr[...].astype(F32)
    for h in range(2):
        deliver(h).wait_recv()
        for i in range(half_width // min(unit, half_width)):
            step = min(unit, half_width)
            at = h * half_width + i * step
            state = hst[x * per_sub + at // unit][:, at % unit : at % unit + step]
            total = state.astype(F32) + base[c, :, at : at + step]
            total = total + conr[h, :, i * step : (i + 1) * step].astype(F32)
            out_ref[:, at : at + step] = total.astype(BF16)
    for i in range(2):
        send(ow.at[z, i], ow.at[z, i], d0_s.at[i], d0_r.at[i], sibling).wait_send()
    to_sibling.wait_send()

    def drain(s, carry):
        count_ring(s, z).wait_send()
        swap_a(s - 1).wait_send()
        swap_b(s - 1).wait_send()
        for j in range(SUBS):
            @pl.when(s < half)
            def _():
                for make in (ring1, ring2, pair1, pair2):
                    make(s, j, z).wait_send()

            give(s, j, z).wait_send()

        @pl.when(s < half)
        def _():
            for o in (1, 3):
                over(s, o, xin.at[s, 0]).wait_send()
            count_pair(s, z).wait_send()
            for b in range(2):
                ring_z(s, b).wait_send()
                for g in range(2):
                    ring_p(s, b, g).wait_send()

        return carry

    lax.fori_loop(1, half + 1, drain, 0)
    for k in range(2):
        j = sub_at(k)
        for make in (ring1, pair1):
            make(half, j, z).wait_send()
        ring2(half, rows_at(unit_at(1 - half), 2 * (1 - c) + k), z).wait_send()
        pair2(half, own_far[k], z).wait_send()
        deliver(k).wait_send()
        swap_z(k).wait_send()
        over(0, 1 + 2 * k, xin.at[0, 0]).wait_send()
        over_far(1 + 2 * k).wait_send()
    for j in range(SUBS):
        send(own.at[j], oth.at[j], ot_s.at[j], ot_r.at[j], sibling).wait_send()
    for o in (1, 2, 3):
        spread(o).wait_send()
    for g in range(2):
        ring_p(0, c, g).wait_send()
    ring_z(0, c).wait_send()
    swap_p.wait_send()


def per_device(nz, *args):
    (queries, keys, values, out_weight, residual, gain, ids, slots, weights, w_gate, w_up, w_down) = args
    block, heads_width = queries.shape
    d_model = residual.shape[1]
    width = d_model // SUBS
    half = nz // 2
    lane = out_weight.shape[1]
    ow_rows = out_weight.shape[0] // 2
    unit_rows = 2 * GCAP
    ffw = w_gate.shape[2]
    w_gate, w_up = (jnp.swapaxes(w, 1, 2) for w in (w_gate, w_up))
    vmem = pl.BlockSpec(memory_space=pltpu.VMEM)
    hbm = pl.BlockSpec(memory_space=pl.ANY)
    dma = pltpu.SemaphoreType.DMA
    swap = pltpu.VMEM((half, block, 4 * lane), BF16)
    sub = pltpu.VMEM((SUBS, unit_rows, width), BF16)
    scratch = [
        pltpu.VMEM(keys.shape[1:], BF16),
        pltpu.VMEM(values.shape[1:], BF16),
        pltpu.VMEM(residual.shape, BF16),
        pltpu.VMEM((2, d_model, ffw), BF16),
        pltpu.VMEM((2, d_model, ffw), BF16),
        pltpu.VMEM(w_down.shape, BF16),
        pltpu.VMEM((2, 2, ffw, width), BF16),
        pltpu.VMEM((block, heads_width), BF16),
        pltpu.VMEM((nz, SUBS, ow_rows, lane), BF16),
        swap,
        swap,
        swap,
        swap,
        pltpu.VMEM((nz, block, 2 * lane), BF16),
        sub,
        sub,
        pltpu.VMEM((nz, SUBS, unit_rows, width), BF16),
        pltpu.VMEM((nz, 2, 16, 128), BF16),
        pltpu.VMEM((4, 2 * unit_rows, ffw), F32),
        pltpu.VMEM((3, 2, 2 * unit_rows, ffw), BF16),
        pltpu.VMEM((nz, SUBS, unit_rows, width), BF16),
        pltpu.VMEM((half, SUBS, unit_rows, width), BF16),
        pltpu.VMEM((half + 1, 2, unit_rows, width), BF16),
        pltpu.VMEM((half, 2, block, width), BF16),
        pltpu.VMEM((half, 2, block, width), BF16),
        pltpu.VMEM((half, 2, unit_rows, width // 2), BF16),
        pltpu.VMEM((2, block, width), F32),
        *[pltpu.VMEM((block, width), BF16)] * 2,
        *[pltpu.VMEM((2, unit_rows, width // 2), BF16)] * 2,
        *[pltpu.VMEM((2, block, width // 2), BF16)] * 2,
        pltpu.VMEM((block, 2 * lane), BF16),
        pltpu.VMEM((3, block, 2 * lane), BF16),
        pltpu.VMEM((2, block, unit_rows), BF16),
        dma((6,)),
        dma((2, 2)),
        dma((2,)),
        dma((2,)),
        *[dma((half + 1, SUBS))] * 4,
        *[dma((half,))] * 4,
        *[dma((SUBS,))] * 2,
        *[dma((half + 1, SUBS))] * 4,
        *[dma((1,))] * 2,
        *[dma((half + 1,))] * 4,
        *[dma((half, SUBS))] * 2,
        *[dma((half + 1, 2))] * 2,
        *[dma((half, 6))] * 2,
        *[dma((3,))] * 2,
        *[dma((2,))] * 2,
        *[dma((3,))] * 2,
    ]
    return pl.pallas_call(
        functools.partial(layer_kernel, nz),
        out_shape=jax.ShapeDtypeStruct((block, width), BF16),
        in_specs=[vmem, hbm, hbm, hbm, hbm, vmem, vmem, vmem, vmem, hbm, hbm, hbm],
        out_specs=vmem,
        scratch_shapes=scratch,
        compiler_params=pltpu.CompilerParams(
            collective_id=0, has_side_effects=True, vmem_limit_bytes=67043328
        ),
    )(queries, keys, values, out_weight, residual, gain.reshape(1, -1), ids.T, slots.T, weights.T, w_gate, w_up, w_down)


def solution(mesh):
    in_specs = (
        P(("groups", "fsdp"), "expert"),
        P(("groups", "fsdp"), None, "expert"),
        P(("groups", "fsdp"), None, "expert"),
        P("expert", "fsdp"),
        P(("groups", "fsdp"), None),
        P(),
        P(("groups", "fsdp"), None),
        P(("groups", "fsdp"), None),
        P(("groups", "fsdp"), None),
        P("expert", None, "fsdp"),
        P("expert", None, "fsdp"),
        P("expert", "fsdp", None),
    )
    return jax.shard_map(
        functools.partial(per_device, mesh.shape["fsdp"] // 2),
        mesh=mesh,
        in_specs=in_specs,
        out_specs=P(("groups", "fsdp"), "expert"),
        check_vma=False,
    )
```

```python
import functools

import jax
import jax.numpy as jnp
from jax import lax
from jax.experimental import pallas as pl
from jax.experimental.pallas import tpu as pltpu
from jax.sharding import PartitionSpec as P

HEAD_DIM = 128
GCAP = 36
SUBS = 4
EPS = 1e-05
MESH = pl.DeviceIdType.MESH
F32 = jnp.float32
BF16 = jnp.bfloat16


def dot(a, b):
    return jnp.dot(a, b, preferred_element_type=F32)


def layer_kernel(
    nz,
    q_ref,
    k_hbm,
    v_hbm,
    ow_hbm,
    res_hbm,
    gain_ref,
    ids_ref,
    slots_ref,
    weights_ref,
    wg_hbm,
    wu_hbm,
    wd_hbm,
    out_ref,
    keys,
    vals,
    res,
    wg,
    wu,
    wd,
    stage,
    heads,
    ow,
    xa,
    xar,
    xb,
    xbr,
    hst,
    own,
    oth,
    rows,
    cnt,
    acc,
    hid,
    part,
    dbuf,
    xin,
    pos,
    posr,
    zsr,
    base,
    finp,
    finpr,
    finz,
    finzr,
    con,
    conr,
    xh,
    xhr,
    mix,
    lsem,
    wsem,
    d0_s,
    d0_r,
    r1_s,
    r1_r,
    d1_s,
    d1_r,
    xa_s,
    xa_r,
    xb_s,
    xb_r,
    ot_s,
    ot_r,
    r2_s,
    r2_r,
    d2_s,
    d2_r,
    c0_s,
    c0_r,
    cr_s,
    cr_r,
    cd_s,
    cd_r,
    db_s,
    db_r,
    xi_s,
    xi_r,
    rs_s,
    rs_r,
    fi_s,
    fi_r,
    co_s,
    co_r,
    xh_s,
    xh_r,
):
    half = nz // 2
    half_width = zsr.shape[3]
    n2 = lax.axis_index("fsdp")
    c = lax.rem(n2, 2)
    z = n2 // 2
    x = lax.axis_index("expert")
    step_dir = 2 * c - 1
    ring_next = {"fsdp": lax.rem(z + step_dir + nz, nz) * 2 + c}
    ring_prev = {"fsdp": lax.rem(z - step_dir + nz, nz) * 2 + c}
    sibling = {"fsdp": z * 2 + 1 - c}
    x_first = {"expert": x + 1 - 2 * lax.rem(x, 2)}
    x_second = {"expert": 3 - x}
    x_other = [{"expert": lax.rem(x + o, 4)} for o in range(4)]

    def unit_at(s):
        return lax.rem(z + s * step_dir + 2 * nz, nz)

    def sub_at(k):
        return lax.rem(2 * c + k, SUBS)

    def send(src, dst, s_sem, r_sem, device):
        return pltpu.make_async_remote_copy(
            src_ref=src, dst_ref=dst, send_sem=s_sem, recv_sem=r_sem,
            device_id=device, device_id_type=MESH,
        )

    def ring1(s, j, u):
        ref = ow.at[u, j]
        return send(ref, ref, r1_s.at[s, j], r1_r.at[s, j], ring_next)

    def pair1(s, j, u):
        ref = ow.at[u, j]
        return send(ref, ref, d1_s.at[s, j], d1_r.at[s, j], sibling)

    def ring2(s, j, u):
        ref = rows.at[u, j]
        return send(ref, ref, r2_s.at[s, j], r2_r.at[s, j], ring_next)

    def pair2(s, j, u):
        ref = rows.at[u, j]
        return send(ref, ref, d2_s.at[s, j], d2_r.at[s, j], sibling)

    def count_ring(s, u):
        return send(cnt.at[u], cnt.at[u], cr_s.at[s], cr_r.at[s], ring_next)

    def count_pair(s, u):
        return send(cnt.at[u], cnt.at[u], cd_s.at[s], cd_r.at[s], sibling)

    def swap_a(s):
        return send(xa.at[s], xar.at[s], xa_s.at[s], xa_r.at[s], x_first)

    def swap_b(s):
        return send(xb.at[s], xbr.at[s], xb_s.at[s], xb_r.at[s], x_second)

    def give(s, j, u):
        return send(part.at[u, j], dbuf.at[s - 1, j], db_s.at[s - 1, j], db_r.at[s - 1, j], sibling)

    def quarter_at(o):
        return lax.rem(x + o, 4)

    def lanes(h):
        return pl.ds(pl.multiple_of(h * half_width, half_width), half_width)

    def ring_p(t, b, g):
        sems = rs_s.at[t, 2 * b + g], rs_r.at[t, 2 * b + g]
        cols = pl.ds(g * half_width, half_width)
        src = pos.at[half - t - 1, b, :, cols]
        return send(src, posr.at[t, b, :, cols], *sems, ring_next)

    def ring_z(t, h):
        sems = rs_s.at[t, 4 + h], rs_r.at[t, 4 + h]
        src = dbuf.at[half - t - 1, quarter_at(2), :, lanes(h)]
        return send(src, zsr.at[t, h], *sems, ring_next)

    def over_far(o):
        i = 1 if o == 1 else 0
        part_rows = pl.ds(pl.multiple_of(32 * c, 32), 40)
        src = dbuf.at[half - 1, quarter_at(o), part_rows]
        dst = xin.at[half, i, part_rows]
        return send(src, dst, xi_s.at[half, i], xi_r.at[half, i], x_other[o])

    def over(s, o, src):
        i = 1 if o == 1 else 0
        return send(src, xin.at[s, i], xi_s.at[s, i], xi_r.at[s, i], x_other[o])

    own_rows = ow_hbm.shape[0] // 2
    loads = [
        pltpu.make_async_copy(ow_hbm.at[pl.ds(0, own_rows)], ow.at[z, 2 * c], lsem.at[0]),
        pltpu.make_async_copy(ow_hbm.at[pl.ds(own_rows, own_rows)], ow.at[z, 2 * c + 1], lsem.at[1]),
        pltpu.make_async_copy(k_hbm.at[0], keys, lsem.at[2]),
        pltpu.make_async_copy(v_hbm.at[0], vals, lsem.at[3]),
        pltpu.make_async_copy(res_hbm, res, lsem.at[4]),
        pltpu.make_async_copy(wd_hbm, wd, lsem.at[5]),
    ]

    slabs = 2 * SUBS
    slab_width = stage.shape[3]

    def slab_load(m, i):
        cols = pl.ds(pl.multiple_of((i % SUBS) * slab_width, slab_width), slab_width)
        src = (wg_hbm, wu_hbm)[m].at[i // SUBS, :, cols]
        return pltpu.make_async_copy(src, stage.at[m, i % 2], wsem.at[m, i % 2])

    def turn_slab(m, i):
        slab_load(m, i).wait()
        at = pl.ds(pl.multiple_of((i % SUBS) * slab_width, slab_width), slab_width)
        (wg, wu)[m][i // SUBS, at, :] = jnp.transpose(stage[m, i % 2])

        @pl.when(i + 2 < slabs)
        def _():
            slab_load(m, i + 2).start()

    for load in loads[:5]:
        load.start()
    for i in range(2):
        for m in range(2):
            slab_load(m, jnp.int32(i)).start()
    loads[5].start()

    xin[half] = jnp.zeros(xin.shape[1:], BF16)
    barrier = pltpu.get_barrier_semaphore()
    partners = [ring_next, ring_prev, sibling, *x_other[1:]]
    for device in partners:
        pl.semaphore_signal(barrier, inc=1, device_id=device, device_id_type=MESH)
    pl.semaphore_wait(barrier, len(partners))

    loads[0].wait()
    loads[1].wait()
    for i in range(2):
        j = 2 * c + i
        send(ow.at[z, j], ow.at[z, j], d0_s.at[i], d0_r.at[i], sibling).start()
        ring1(1, j, z).start()
    for i in range(2):
        j = 2 * (1 - c) + i
        send(ow.at[z, j], ow.at[z, j], d0_s.at[i], d0_r.at[i], sibling).wait_recv()
        ring1(1, j, z).start()

    loads[2].wait()
    loads[3].wait()
    block, heads_width = q_ref.shape
    context = keys.shape[0]
    key_pos = lax.broadcasted_iota(jnp.int32, (block, context), 1)
    query_pos = context - block + lax.broadcasted_iota(jnp.int32, (block, context), 0)
    allowed = key_pos <= query_pos
    for h in range(heads_width // HEAD_DIM):
        cols = slice(h * HEAD_DIM, (h + 1) * HEAD_DIM)
        scores = lax.dot_general(
            q_ref[:, cols], keys[...], (((1,), (1,)), ((), ())), preferred_element_type=F32
        ) * HEAD_DIM ** (-0.5)
        masked = jnp.where(allowed, scores, -1e30)
        highest = jnp.max(masked, axis=-1, keepdims=True)
        weights = jnp.where(allowed, jnp.exp(masked - highest), 0.0)
        probs = (weights / jnp.sum(weights, axis=-1, keepdims=True)).astype(BF16)
        heads[:, cols] = dot(probs, vals[...]).astype(BF16)

    unit = 2 * ow.shape[3]
    lane = ow.shape[3]

    def project(s):
        for side, u in enumerate((unit_at(-s), unit_at(s))):
            for b in range(2):
                total = dot(heads[:, :own_rows], ow[u, 2 * b]) + dot(
                    heads[:, own_rows:], ow[u, 2 * b + 1]
                )
                at = side * unit + b * lane
                xa[s, :, at : at + lane] = total.astype(BF16)
        swap_a(s).start()

    def add_first(s):
        swap_a(s).wait_recv()
        xb[s] = (xa[s].astype(F32) + xar[s].astype(F32)).astype(BF16)
        swap_b(s).start()

    def add_second(s):
        swap_b(s).wait_recv()
        for side, u in enumerate((unit_at(-s), unit_at(s))):
            cols = slice(side * unit, (side + 1) * unit)
            attn = xb[s, :, cols].astype(F32) + xbr[s, :, cols].astype(F32)
            left = pl.ds(pl.multiple_of(u * unit, unit), unit)
            hst[u] = (res[:, left].astype(F32) + attn).astype(BF16)

    first_expert = 2 * x
    ids = ids_ref[...]
    within = ids - first_expert
    in_group = (within >= 0) & (within < 2)
    is_first = jnp.where(ids == first_expert, 1.0, 0.0)
    lead = jnp.sum(jnp.sum(is_first, axis=1, keepdims=True), axis=0, keepdims=True)
    target = jnp.where(in_group, slots_ref[...] + within * lead.astype(jnp.int32) + GCAP * c, -1)
    row_ids = lax.broadcasted_iota(jnp.int32, (2 * GCAP, block), 0)
    picks = [row_ids == target[k : k + 1, :] for k in range(2)]
    picked = picks[0] | picks[1]
    one_hot = jnp.where(picked, 1.0, 0.0).astype(BF16)
    share = weights_ref[...].astype(F32) / 65536.0
    share_high = share.astype(BF16).astype(F32)
    facts = [share_high[0:1], share_high[1:2], share[0:1] - share_high[0:1], share[1:2] - share_high[1:2]]
    for o in (3, 1, 0):
        other = 2 * lax.rem(x + o, 4)
        inside = (ids >= other) & (ids < other + 2)
        count = jnp.where(ids == other, 1.0, 0.0)
        count = jnp.sum(jnp.sum(count, axis=1, keepdims=True), axis=0, keepdims=True)
        place = slots_ref[...] + (ids - other) * count.astype(jnp.int32) + GCAP * c + 1
        place = jnp.where(inside, place, 0).astype(F32)
        facts = [place[0:1], place[1:2]] + facts
    shift = (block, cnt.shape[3])
    spot = lax.broadcasted_iota(jnp.int32, shift, 0) + block * c
    placed = spot == lax.broadcasted_iota(jnp.int32, shift, 1)
    same = (
        lax.broadcasted_iota(jnp.int32, (block, block), 0)
        == lax.broadcasted_iota(jnp.int32, (block, block), 1)
    )
    line = lax.broadcasted_iota(jnp.int32, cnt.shape[2:], 0)
    info = jnp.zeros(cnt.shape[2:], F32)
    for i, fact in enumerate(facts):
        column = jnp.sum(jnp.where(same, fact, 0.0), axis=1, keepdims=True)
        wide_fact = jnp.sum(jnp.where(placed, column, 0.0), axis=0, keepdims=True)
        info = jnp.where(line == i + 2, wide_fact, info)
    mixed = jnp.where(picks[0], share[0:1, :], 0.0) + jnp.where(picks[1], share[1:2, :], 0.0)
    high = mixed.astype(BF16)
    low = (mixed - high.astype(F32)).astype(BF16)
    turn = jnp.where(same, 1.0, 0.0).astype(BF16)
    for i, piece in enumerate((high, low)):
        mix[i] = lax.dot_general(
            turn, piece, (((1,), (1,)), ((), ())), preferred_element_type=F32
        ).astype(BF16)
    loads[4].wait()

    def take_pair(s):
        for j in range(SUBS):
            pair1(s, j, unit_at(s)).wait_recv()

    def projection_step(s, carry):
        u = unit_at(-s)
        for k in range(SUBS):
            j = sub_at(k)
            ring1(s, j, u).wait_recv()
            if k < 2:
                ring1(s + 1, j, u).start()
            else:
                @pl.when(s < half - 1)
                def _():
                    ring1(s + 1, j, u).start()
            pair1(s, j, u).start()
            if k in (0, 2):
                turn_slab(k // 2, s - 1)
            if k == 1:
                @pl.when(s >= 2)
                def _():
                    take_pair(s - 1)

                project(s - 1)

                @pl.when(s >= 2)
                def _():
                    add_first(s - 2)

                @pl.when(s >= 3)
                def _():
                    add_second(s - 3)

        return carry

    lax.fori_loop(1, half, projection_step, 0)
    u = unit_at(half)
    ring1(half, sub_at(0), u).wait_recv()
    pair1(half, sub_at(0), u).start()
    take_pair(half - 1)
    project(half - 1)
    ring1(half, sub_at(1), u).wait_recv()
    pair1(half, sub_at(1), u).start()
    add_first(half - 2)
    if half >= 3:
        add_second(half - 3)
    width = rows.shape[3]
    per_sub = width // unit
    d_model = width * SUBS

    def rows_at(u, k):
        return lax.rem(lax.rem(u + half + 1, nz) // per_sub + 1 + k, SUBS)

    def trade(j):
        return send(own.at[j], oth.at[j], ot_s.at[j], ot_r.at[j], sibling)

    def dispatch(k):
        j = rows_at(z, k)
        for i in range(per_sub):
            u = j * per_sub + i
            gain = gain_ref[:, pl.ds(pl.multiple_of(u * unit, unit), unit)]
            scaled = (hst[u].astype(F32) * gain).astype(BF16)
            own[j, :, i * unit : (i + 1) * unit] = dot(one_hot, scaled).astype(BF16)
        trade(j).start()

    def launch(k):
        j = rows_at(z, k)
        trade(j).wait_recv()
        rows[z, j] = own[j] + oth[j]
        ring2(1, j, z).start()

    far = unit_at(half)
    for k in range(2, 4):
        pair1(half, sub_at(k), far).wait_recv()
    for b in range(2):
        total = dot(heads[:, :own_rows], ow[far, 2 * b]) + dot(
            heads[:, own_rows:], ow[far, 2 * b + 1]
        )
        xh[:, b * lane : (b + 1) * lane] = total.astype(BF16)

    def spread(o):
        return send(xh, xhr.at[o - 1], xh_s.at[o - 1], xh_r.at[o - 1], x_other[o])

    for o in (2, 1, 3):
        spread(o).start()
    add_first(half - 1)
    add_second(half - 2)
    dispatch(0)
    dispatch(1)
    launch(0)
    launch(1)
    add_second(half - 1)
    for i in range(half - 1, slabs):
        for m in range(2):
            turn_slab(m, jnp.int32(i))
    for o in (1, 3, 2):
        spread(o).wait_recv()
    near = 2 - 2 * lax.rem(x, 2)
    first = xh[...].astype(F32) + xhr[near].astype(F32)
    attn = first + (xhr[1].astype(F32) + xhr[2 - near].astype(F32))
    left = pl.ds(pl.multiple_of(far * unit, unit), unit)
    hst[far] = (res[:, left].astype(F32) + attn).astype(BF16)
    dispatch(2)
    dispatch(3)
    square = jnp.zeros((block, 1), F32)
    for i in range(nz):
        state = hst[i].astype(F32)
        square = square + jnp.sum(state * state, axis=-1, keepdims=True)
    scale = lax.rsqrt(square / d_model + EPS)
    by_position = jnp.sum(jnp.where(same, scale, 0.0), axis=0, keepdims=True)
    by_row = jnp.sum(jnp.where(picked, by_position, 0.0), axis=1, keepdims=True)
    grid = (2 * GCAP, cnt.shape[3])
    diagonal = lax.broadcasted_iota(jnp.int32, grid, 0) == lax.broadcasted_iota(jnp.int32, grid, 1)
    row_scale = jnp.sum(jnp.where(diagonal, by_row, 0.0), axis=0, keepdims=True)
    scale_high = row_scale.astype(BF16).astype(F32)
    info = jnp.where(line == 12, row_scale - scale_high, info)
    cnt[z, c] = jnp.where(line == 0, lead, jnp.where(line == 1, scale_high, info)).astype(BF16)
    to_sibling = send(cnt.at[z, c], cnt.at[z, c], c0_s.at[0], c0_r.at[0], sibling)
    to_sibling.start()
    launch(2)
    launch(3)
    send(cnt.at[z, 1 - c], cnt.at[z, 1 - c], c0_s.at[0], c0_r.at[0], sibling).wait_recv()
    count_ring(1, z).start()
    for load in loads[5:]:
        load.wait()
    unit_rows = 2 * GCAP
    ffw = wg.shape[2]
    quarter = width // SUBS

    def arrive_count(s, last):
        u = unit_at(-s)
        count_ring(s, u).wait_recv()
        if not last:
            count_ring(s + 1, u).start()
            count_pair(s, u).start()

    def gate_up(j, units, first):
        slab = pl.ds(j * width, width) if isinstance(j, int) else pl.ds(
            pl.multiple_of(j * width, width), width
        )
        block_rows = jnp.concatenate([rows[u, j] for u in units], axis=0)
        many = len(units) * unit_rows
        for i in range(4):
            weight = (wg, wu)[i // 2]
            total = dot(block_rows, weight[i % 2, slab, :])
            if first:
                acc[i, :many] = total
            else:
                acc[i, :many] += total

    def activate(slot, units):
        many = len(units) * unit_rows
        row = lax.broadcasted_iota(jnp.int32, (many, ffw), 0).astype(F32)
        facts = [[cnt[u, b].astype(F32) for b in range(2)] for u in units]
        limit = facts[0][0][0:1, 0:1]
        place = row
        for i in range(1, 2 * len(units)):
            later = row >= i * GCAP
            limit = jnp.where(later, facts[i // 2][i % 2][0:1, 0:1], limit)
            place = jnp.where(later, row - i * GCAP, place)
        second = place >= limit
        wide = (many, cnt.shape[3])
        at = lax.broadcasted_iota(jnp.int32, wide, 0) - lax.broadcasted_iota(jnp.int32, wide, 1)
        factor = jnp.zeros(wide, F32)
        for i, u in enumerate(units):
            known = facts[i][0] + facts[i][1]
            row_scale = known[1:2] + known[12:13]
            factor = factor + jnp.where(at == i * unit_rows, row_scale, 0.0)
        factor = jnp.sum(factor, axis=1, keepdims=True)
        for e in range(2):
            g, up = acc[e, :many] * factor, acc[2 + e, :many] * factor
            value = g / (1.0 + jnp.exp(-g)) * up
            mine = second if e == 1 else jnp.logical_not(second)
            hid[slot, e, :many] = jnp.where(mine, value, 0.0).astype(BF16)

    def down(slot, f, units):
        many = len(units) * unit_rows
        for i in range(SUBS):
            start = f * width + i * quarter
            if not isinstance(f, int):
                start = pl.multiple_of(start, quarter)
            cols = pl.ds(start, quarter)
            total = dot(hid[slot, 0, :many], wd[0, :, cols]) + dot(hid[slot, 1, :many], wd[1, :, cols])
            for n, u in enumerate(units):
                part[u, f, :, i * quarter : (i + 1) * quarter] = total[
                    n * unit_rows : (n + 1) * unit_rows
                ].astype(BF16)

    def both(s):
        return (unit_at(-s), unit_at(s))

    def prepare(s, last=False):
        u = unit_at(s)
        for o in (1, 3, 2, 0):
            f = quarter_at(o)
            give(s, f, u).wait_recv()
            dbuf[s - 1, f] = (part[u, f].astype(F32) + dbuf[s - 1, f].astype(F32)).astype(BF16)
            if o in (1, 3):
                (over_far(o) if last else over(s, o, dbuf.at[s - 1, f])).start()

    def by_positions(s, mine, last=False):
        for o in (1, 3):
            (over_far(o) if last else over(s, o, xin.at[s, 0])).wait_recv()
        u = unit_at(s)
        facts = cnt[u, 0].astype(F32) + cnt[u, 1].astype(F32)
        row = lax.broadcasted_iota(jnp.int32, (unit_rows, cnt.shape[3]), 0).astype(F32) + 1.0
        highs, lows = [], []
        for i in range(3):
            hit = [row == facts[2 + 2 * i + k : 3 + 2 * i + k] for k in range(2)]
            for kept, at in ((highs, 8), (lows, 10)):
                kept.append(
                    jnp.where(hit[0], facts[at : at + 1], 0.0)
                    + jnp.where(hit[1], facts[at + 1 : at + 2], 0.0)
                )
        sums = jnp.concatenate([mine, xin[s, 0], xin[s, 1]], axis=0)
        total = None
        for weight in (highs, lows):
            turned = jnp.transpose(jnp.concatenate(weight, axis=0)).astype(BF16)
            term = dot(turned, sums)
            total = term if total is None else total + term
        return total

    def gather_positions(s, last=False):
        total = by_positions(s, dbuf[s - 1, x], last)
        for b in range(2):
            pos[s - 1, b] = total[b * block : (b + 1) * block].astype(BF16)

    def sum_p(t, b, arrived):
        at = half - t - 1
        for g in range(2):
            if arrived:
                ring_p(t - 1, b, g).wait_recv()
                cols = slice(g * half_width, (g + 1) * half_width)
                total = pos[at, b, :, cols].astype(F32) + posr[t - 1, b, :, cols].astype(F32)
                pos[at, b, :, cols] = total.astype(BF16)
            ring_p(t, b, g).start()

    def sum_z(t, h, arrived):
        if arrived:
            ring_z(t - 1, h).wait_recv()
            at = half - t - 1
            f = quarter_at(2)
            dbuf[at, f, :, lanes(h)] = (
                dbuf[at, f, :, lanes(h)].astype(F32) + zsr[t - 1, h].astype(F32)
            ).astype(BF16)
        ring_z(t, h).start()

    def expert_step(s, carry):
        u = unit_at(-s)
        for k in range(SUBS):
            j = rows_at(u, k)
            ring2(s, j, u).wait_recv()

            @pl.when((s < half - 1) | (c == 1 if k < 2 else c == 0))
            def _():
                ring2(s + 1, j, u).start()

            pair2(s, j, u).start()
            if k == 2:
                arrive_count(s, False)
            @pl.when(s >= 2)
            def _():
                pair2(s - 1, k, unit_at(s - 1)).wait_recv()

            gate_up(k, both(s - 1), k == 0)
            if k == SUBS - 1:
                @pl.when(s >= 2)
                def _():
                    count_pair(s - 1, unit_at(s - 1)).wait_recv()

                activate(lax.rem(s - 1, 3), both(s - 1))

            @pl.when(s >= 2)
            def _():
                down(lax.rem(s - 2, 3), k, both(s - 2))

            @pl.when(s >= 3)
            def _():
                give(s - 2, k, unit_at(2 - s)).start()

        @pl.when(s == 3)
        def _():
            for o in (1, 3):
                over(0, o, part.at[z, quarter_at(o)]).start()

        @pl.when(s >= 4)
        def _():
            prepare(s - 3)

        return carry

    lax.fori_loop(1, half, expert_step, 0)

    own_far = [rows_at(far, 2 * (1 - c) + i) for i in range(2)]
    other_far = [rows_at(far, 2 * c + i) for i in range(2)]
    prepare(half - 3)
    for k in range(SUBS):
        pair2(half - 1, k, unit_at(half - 1)).wait_recv()
        if k == SUBS - 1:
            ring2(half, own_far[0], far).wait_recv()
            pair2(half, own_far[0], far).start()
        gate_up(k, both(half - 1), k == 0)
    count_pair(half - 1, unit_at(half - 1)).wait_recv()
    activate((half - 1) % 3, both(half - 1))
    for o in (1, 3, 2, 0):
        down((half - 1) % 3, quarter_at(o), both(half - 1))
        give(half - 1, quarter_at(o), unit_at(1 - half)).start()
    ring2(half, own_far[1], far).wait_recv()
    pair2(half, own_far[1], far).start()
    arrive_count(half, True)

    prepare(half - 1)
    sum_z(1, 1 - c, False)
    single = (far,)
    for i in range(2):
        gate_up(own_far[i], single, i == 0)
    for i in range(2):
        pair2(half, other_far[i], far).wait_recv()
        gate_up(other_far[i], single, False)
    activate(half % 3, single)
    for o in (1, 3, 2, 0):
        down(half % 3, quarter_at(o), single)
        give(half, quarter_at(o), far).start()
    for o in (1, 3, 2, 0):
        down((half - 2) % 3, quarter_at(o), both(half - 2))
        give(half - 2, quarter_at(o), unit_at(2 - half)).start()
    prepare(half, True)
    sum_z(0, c, False)
    gather_positions(half - 1)
    sum_p(1, 1 - c, False)
    prepare(half - 2)
    sum_z(2, 1 - c, True)
    gather_positions(half, True)
    sum_p(0, c, False)
    sum_z(1, c, True)
    total = by_positions(0, part[z, x])
    for b in range(2):
        base[b] = total[b * block : (b + 1) * block]

    def sum_step(t, carry):
        @pl.when(t < half)
        def _():
            sum_z(t, 1 - c, True)

        sum_z(t - 1, c, True)
        sum_p(t - 2, c, True)
        gather_positions(half - t + 1)
        sum_p(t - 1, 1 - c, True)
        return carry

    lax.fori_loop(3, half + 1, sum_step, 0)

    def swap_z(h):
        return send(finz.at[h], finzr.at[h], fi_s.at[h], fi_r.at[h], sibling)

    swap_p = send(finp, finpr, fi_s.at[2], fi_r.at[2], sibling)

    def close_z(h):
        ring_z(half - 1, h).wait_recv()
        own_part = part[z, quarter_at(2), :, lanes(h)]
        finz[h] = (own_part.astype(F32) + zsr[half - 1, h].astype(F32)).astype(BF16)
        swap_z(h).start()

    def deliver(h):
        return send(con.at[h], conr.at[h], co_s.at[h], co_r.at[h], x_other[2])

    def cross(h):
        swap_z(h).wait_recv()
        total = (finz[h].astype(F32) + finzr[h].astype(F32)).astype(BF16)
        con[h] = (dot(mix[0], total) + dot(mix[1], total)).astype(BF16)
        deliver(h).start()

    close_z(1 - c)
    close_z(c)
    cross(0)
    cross(1)
    sum_p(half - 1, c, True)
    for g in range(2):
        ring_p(half - 1, 1 - c, g).wait_recv()
    finp[...] = (base[1 - c] + posr[half - 1, 1 - c].astype(F32)).astype(BF16)
    swap_p.start()
    for i in range(2):
        send(ow.at[z, i], ow.at[z, i], d0_s.at[i], d0_r.at[i], sibling).wait_send()
    to_sibling.wait_send()

    def drain(s, carry):
        count_ring(s, z).wait_send()
        swap_a(s - 1).wait_send()
        swap_b(s - 1).wait_send()
        for j in range(SUBS):
            @pl.when(s < half)
            def _():
                for make in (ring1, ring2, pair1, pair2):
                    make(s, j, z).wait_send()

            give(s, j, z).wait_send()

        @pl.when(s < half)
        def _():
            for o in (1, 3):
                over(s, o, xin.at[s, 0]).wait_send()
            count_pair(s, z).wait_send()
            for b in range(2):
                ring_z(s, b).wait_send()
                for g in range(2):
                    ring_p(s, b, g).wait_send()

        return carry

    lax.fori_loop(1, half + 1, drain, 0)
    for k in range(2):
        j = sub_at(k)
        for make in (ring1, pair1):
            make(half, j, z).wait_send()
        ring2(half, rows_at(unit_at(1 - half), 2 * (1 - c) + k), z).wait_send()
        pair2(half, own_far[k], z).wait_send()
        deliver(k).wait_send()
        swap_z(k).wait_send()
        over(0, 1 + 2 * k, xin.at[0, 0]).wait_send()
        over_far(1 + 2 * k).wait_send()
    for j in range(SUBS):
        send(own.at[j], oth.at[j], ot_s.at[j], ot_r.at[j], sibling).wait_send()
    for o in (1, 2, 3):
        spread(o).wait_send()
    for g in range(2):
        ring_p(0, c, g).wait_send()
    ring_z(0, c).wait_send()
    swap_p.wait_send()

    for g in range(2):
        ring_p(half - 1, c, g).wait_recv()
    swap_p.wait_recv()
    base[c] = base[c] + posr[half - 1, c].astype(F32) + finpr[...].astype(F32)
    for h in range(2):
        deliver(h).wait_recv()
        for i in range(half_width // min(unit, half_width)):
            step = min(unit, half_width)
            at = h * half_width + i * step
            state = hst[x * per_sub + at // unit][:, at % unit : at % unit + step]
            total = state.astype(F32) + base[c, :, at : at + step]
            total = total + conr[h, :, i * step : (i + 1) * step].astype(F32)
            out_ref[:, at : at + step] = total.astype(BF16)


def per_device(nz, *args):
    (queries, keys, values, out_weight, residual, gain, ids, slots, weights, w_gate, w_up, w_down) = args
    block, heads_width = queries.shape
    d_model = residual.shape[1]
    width = d_model // SUBS
    half = nz // 2
    lane = out_weight.shape[1]
    ow_rows = out_weight.shape[0] // 2
    unit_rows = 2 * GCAP
    ffw = w_gate.shape[2]
    w_gate, w_up = (jnp.swapaxes(w, 1, 2) for w in (w_gate, w_up))
    vmem = pl.BlockSpec(memory_space=pltpu.VMEM)
    hbm = pl.BlockSpec(memory_space=pl.ANY)
    dma = pltpu.SemaphoreType.DMA
    swap = pltpu.VMEM((half, block, 4 * lane), BF16)
    sub = pltpu.VMEM((SUBS, unit_rows, width), BF16)
    scratch = [
        pltpu.VMEM(keys.shape[1:], BF16),
        pltpu.VMEM(values.shape[1:], BF16),
        pltpu.VMEM(residual.shape, BF16),
        pltpu.VMEM((2, d_model, ffw), BF16),
        pltpu.VMEM((2, d_model, ffw), BF16),
        pltpu.VMEM(w_down.shape, BF16),
        pltpu.VMEM((2, 2, ffw, width), BF16),
        pltpu.VMEM((block, heads_width), BF16),
        pltpu.VMEM((nz, SUBS, ow_rows, lane), BF16),
        swap,
        swap,
        swap,
        swap,
        pltpu.VMEM((nz, block, 2 * lane), BF16),
        sub,
        sub,
        pltpu.VMEM((nz, SUBS, unit_rows, width), BF16),
        pltpu.VMEM((nz, 2, 16, 128), BF16),
        pltpu.VMEM((4, 2 * unit_rows, ffw), F32),
        pltpu.VMEM((3, 2, 2 * unit_rows, ffw), BF16),
        pltpu.VMEM((nz, SUBS, unit_rows, width), BF16),
        pltpu.VMEM((half, SUBS, unit_rows, width), BF16),
        pltpu.VMEM((half + 1, 2, unit_rows, width), BF16),
        pltpu.VMEM((half, 2, block, width), BF16),
        pltpu.VMEM((half, 2, block, width), BF16),
        pltpu.VMEM((half, 2, unit_rows, width // 2), BF16),
        pltpu.VMEM((2, block, width), F32),
        *[pltpu.VMEM((block, width), BF16)] * 2,
        *[pltpu.VMEM((2, unit_rows, width // 2), BF16)] * 2,
        *[pltpu.VMEM((2, block, width // 2), BF16)] * 2,
        pltpu.VMEM((block, 2 * lane), BF16),
        pltpu.VMEM((3, block, 2 * lane), BF16),
        pltpu.VMEM((2, block, unit_rows), BF16),
        dma((6,)),
        dma((2, 2)),
        dma((2,)),
        dma((2,)),
        *[dma((half + 1, SUBS))] * 4,
        *[dma((half,))] * 4,
        *[dma((SUBS,))] * 2,
        *[dma((half + 1, SUBS))] * 4,
        *[dma((1,))] * 2,
        *[dma((half + 1,))] * 4,
        *[dma((half, SUBS))] * 2,
        *[dma((half + 1, 2))] * 2,
        *[dma((half, 6))] * 2,
        *[dma((3,))] * 2,
        *[dma((2,))] * 2,
        *[dma((3,))] * 2,
    ]
    return pl.pallas_call(
        functools.partial(layer_kernel, nz),
        out_shape=jax.ShapeDtypeStruct((block, width), BF16),
        in_specs=[vmem, hbm, hbm, hbm, hbm, vmem, vmem, vmem, vmem, hbm, hbm, hbm],
        out_specs=vmem,
        scratch_shapes=scratch,
        compiler_params=pltpu.CompilerParams(
            collective_id=0, has_side_effects=True, vmem_limit_bytes=67043328
        ),
    )(queries, keys, values, out_weight, residual, gain.reshape(1, -1), ids.T, slots.T, weights.T, w_gate, w_up, w_down)


def solution(mesh):
    in_specs = (
        P(("groups", "fsdp"), "expert"),
        P(("groups", "fsdp"), None, "expert"),
        P(("groups", "fsdp"), None, "expert"),
        P("expert", "fsdp"),
        P(("groups", "fsdp"), None),
        P(),
        P(("groups", "fsdp"), None),
        P(("groups", "fsdp"), None),
        P(("groups", "fsdp"), None),
        P("expert", None, "fsdp"),
        P("expert", None, "fsdp"),
        P("expert", "fsdp", None),
    )
    return jax.shard_map(
        functools.partial(per_device, mesh.shape["fsdp"] // 2),
        mesh=mesh,
        in_specs=in_specs,
        out_specs=P(("groups", "fsdp"), "expert"),
        check_vma=False,
    )
```
